32 devices in a mesh: row: 4 (over y, x), col: 8 (over z, core).
Axes of the slice: x: 2, y: 2, z: 4, core: 2. Of those that a mesh axis runs over, the one named last changes fastest.
Arguments:
- inputs: bfloat16 [256, 16384], P('col', 'row'), may hold values from -0.375 to 0.375
- weight: bfloat16 [16384, 18432], P('row', 'col'), may hold values from -0.046875 to 0.046875
- grad_out: bfloat16 [256, 18432], P('row', 'col'), may hold values from -6 to 6
- positions: int32 [256], P('row'), may hold values from 0 to 8191
Outputs:
- input_grad: bfloat16 [256, 16384], P('col', 'row')
- weight_grad: float32 [16384, 18432], P('row', 'col')
The draws below stay inside these ranges and needn't reach their ends.
All inputs are finite; a program needn't handle non-finite values.
Results may differ from the reference program's by a relative error of at most 0.0065.
Values may be sent and summed in bfloat16 or wider, within the bound.
A program may use at most 192 MiB of HBM per device.

```python
import math
import jax
import jax.numpy as jnp
from jax import lax

D = 16384
QHEADS = 128
KVHEADS = 8
HEAD = 128
F = 18432
TOKENS = 256


def set_ends(result, own_key, least, largest):
    dims = result.shape
    place = [jax.random.randint(jax.random.fold_in(own_key, axis), (), 0, dims[axis]) for axis in range(len(dims))]
    result = result.at[tuple(place)].set(least)
    longest = dims.index(max(dims))
    place[longest] = (place[longest] + 1) % dims[longest]
    return result.at[tuple(place)].set(largest)


def block_levels(rng, shape, cuts, least, high):
    gain, own = 1.0, jax.random.fold_in(rng, 6)
    for position, parts in cuts:
        heights = jnp.exp(jax.random.uniform(jax.random.fold_in(own, position), (parts,), jnp.float32, least / len(cuts), high / len(cuts)))
        gain = gain * jnp.repeat(heights, shape[position] // parts).reshape([-1 if axis == position else 1 for axis in range(len(shape))])
    return gain


def centred(key, shape, deviation, bound, shards=(), held_as=jnp.bfloat16):
    loudness = block_levels(key, shape, shards, -0.22, 0.18) if shards else 1.0
    values = jax.random.normal(key, shape, jnp.float32) * deviation * loudness
    return jnp.minimum(jnp.maximum(values, -bound), bound).astype(held_as)


def setup_inputs(seed: int = 0) -> dict:
    key_list = jax.random.split(jax.random.key(seed), 5)
    inputs = centred(key_list[0], (TOKENS, D), (TOKENS ** -0.5), 0.375, ((0, 8), (1, 4)))
    weight = centred(key_list[1], (D, F), D ** -0.5, 0.046875, ((0, 4), (1, 8)))
    grad_out = centred(key_list[2], (TOKENS, F), 1.0, 6.0, ((0, 4), (1, 8)))
    positions = set_ends(jax.random.randint(key_list[3], (TOKENS,), 0, 8192), jax.random.fold_in(key_list[3], 1), 0, 8191).astype(jnp.int32)
    return {"inputs": inputs, "weight": weight, "grad_out": grad_out, "positions": positions}


def scaled_freq(within):
    base = jnp.exp(-(2.0 * within.astype(jnp.float32) / HEAD) * math.log(500000.0))
    wave = 2.0 * math.pi / base
    smooth = (8192.0 / wave - 1.0) / 3.0
    middle = (1.0 - smooth) * base / 8.0 + smooth * base
    return jnp.where(wave < 2048.0, base, jnp.where(wave > 8192.0, base / 8.0, middle))


def unrotate(grad, positions, col_start):
    rows = grad.shape[0]
    pairs = grad.shape[1] // 2
    columns = col_start + 2 * jnp.arange(pairs, dtype=jnp.int32)
    within = (columns % HEAD) // 2
    freq = scaled_freq(within)
    angle = positions.astype(jnp.float32)[:, None] * freq[None, :]
    cosine = jnp.cos(angle)
    sine = jnp.sin(angle)
    rotated = (columns < (QHEADS + KVHEADS) * HEAD)[None, :]
    cosine = jnp.where(rotated, cosine, 1.0)
    sine = jnp.where(rotated, sine, 0.0)
    split = grad.astype(jnp.float32).reshape(rows, pairs, 2)
    first = split[:, :, 0]
    second = split[:, :, 1]
    new_first = first * cosine + second * sine
    new_second = second * cosine - first * sine
    return jnp.stack([new_first, new_second], axis=2).reshape(rows, 2 * pairs).astype(jnp.bfloat16)


def reference(inputs, weight, grad_out, positions):
    grad = unrotate(grad_out, positions, 0)
    input_grad = lax.dot_general(grad, weight, (((1,), (1,)), ((), ())), preferred_element_type=jnp.float32).astype(jnp.bfloat16)
    weight_grad = lax.dot_general(inputs, grad, (((0,), (0,)), ((), ())), preferred_element_type=jnp.float32)
    return input_grad, weight_grad
```

```python
import functools
import math

import jax
import jax.numpy as jnp
from jax import lax
from jax.experimental import pallas as pl
from jax.experimental.pallas import tpu as pltpu
from jax.sharding import PartitionSpec as P

QHEADS = 128
KVHEADS = 8
HEAD = 128
PAIR_LAG = 2
LEVEL_LAG = 3
MESH = pl.DeviceIdType.MESH
half = jnp.bfloat16


def scaled_freq(within):
    base = jnp.exp(-(2.0 * within.astype(jnp.float32) / HEAD) * math.log(500000.0))
    wave = 2.0 * math.pi / base
    smooth = (8192.0 / wave - 1.0) / 3.0
    middle = (1.0 - smooth) * base / 8.0 + smooth * base
    return jnp.where(wave < 2048.0, base, jnp.where(wave > 8192.0, base / 8.0, middle))


def unrotate(grad, positions, col_start):
    width = grad.shape[1]
    lanes = col_start + jnp.arange(HEAD, dtype=jnp.int32)
    freq = scaled_freq(lanes % HEAD // 2)
    angle = positions.astype(jnp.float32)[:, None] * freq[None, :]
    cosine = jnp.cos(angle)
    sine = jnp.where((lanes % 2 == 0)[None, :], jnp.sin(angle), -jnp.sin(angle))
    reps = -(-width // HEAD)
    cosine = jnp.tile(cosine, (1, reps))[:, :width]
    sine = jnp.tile(sine, (1, reps))[:, :width]
    columns = col_start + jnp.arange(width, dtype=jnp.int32)
    rotated = (columns < (QHEADS + KVHEADS) * HEAD)[None, :]
    wide = grad.astype(jnp.float32)
    other = jnp.where(
        (columns % 2 == 0)[None, :], jnp.roll(wide, -1, axis=1), jnp.roll(wide, 1, axis=1)
    )
    return jnp.where(rotated, wide * cosine + other * sine, wide).astype(jnp.bfloat16)


def unrotate_heads(g_ref, pos_ref, out, col_start):
    trow, width = g_ref.shape
    lanes = col_start + lax.broadcasted_iota(jnp.int32, (trow, HEAD), 1)
    freq = scaled_freq((col_start + lax.broadcasted_iota(jnp.int32, (8, HEAD), 1)) % HEAD // 2)[0:1, :]
    row = lax.broadcasted_iota(jnp.int32, (trow, trow), 0)
    lane = lax.broadcasted_iota(jnp.int32, (trow, trow), 1)
    spread = jnp.broadcast_to(pos_ref[...].astype(jnp.float32), (trow, trow))
    column = jnp.sum(jnp.where(row == lane, spread, 0.0), axis=1, keepdims=True)
    angle = column * freq
    even = lanes % 2 == 0
    cosine = jnp.cos(angle)
    sine = jnp.sin(angle)
    sine = jnp.where(even, sine, -sine)
    for first in range(0, width, HEAD):
        wide = g_ref[:, first:first + HEAD].astype(jnp.float32)
        other = jnp.where(even, pltpu.roll(wide, HEAD - 1, 1), pltpu.roll(wide, 1, 1))
        turned = wide * cosine + other * sine
        rotated = lanes + first < (QHEADS + KVHEADS) * HEAD
        out[0:trow, first:first + HEAD] = jnp.where(rotated, turned, wide).astype(jnp.bfloat16)


def exclusive_or(a, b, size):
    total, bit = 0, 1
    while bit < size:
        total = total + bit * ((a // bit % 2 + b // bit % 2) % 2)
        bit *= 2
    return total


def kernel(rows_n, chips, parts, raw, g_ref, pos_ref, x_ref, w_ref, gall, xall, out_ref,
           w_v, pb, rb, ub, db, sb_up, sb_dn,
           w_sem, gs, gr, xs_up, xs_dn, xs_p, xr, xp, ps, pr, us, ur, ds, dr):
    r = lax.axis_index("row")
    q = lax.axis_index("col")
    z, c = q // 2, q % 2
    mate = z * 2 + 1 - c
    up, down = q + 2, q - 2
    trow, tcol = g_ref.shape[0], x_ref.shape[0]
    depth = w_ref.shape[0]
    dc = depth // parts

    def w_copy(h):
        rows = pl.ds(h * dc, dc)
        return pltpu.make_async_copy(w_ref.at[rows], w_v.at[rows], w_sem.at[h])

    for h in range(parts):
        w_copy(h).start()

    if raw:
        unrotate_heads(g_ref, pos_ref, gall, q * g_ref.shape[1])
    else:
        gall[0:trow, :] = g_ref[...]

    barrier = pltpu.get_barrier_semaphore()
    for j in range(1, rows_n):
        pl.semaphore_signal(barrier, inc=1, device_id=(exclusive_or(r, j, rows_n), q), device_id_type=MESH)
    pl.semaphore_signal(barrier, inc=1, device_id=(r, mate), device_id_type=MESH)

    @pl.when(z > 0)
    def _():
        pl.semaphore_signal(barrier, inc=1, device_id=(r, down), device_id_type=MESH)

    @pl.when(z < chips - 1)
    def _():
        pl.semaphore_signal(barrier, inc=1, device_id=(r, up), device_id_type=MESH)

    inner = (z > 0) & (z < chips - 1)

    @pl.when(inner)
    def _():
        pl.semaphore_wait(barrier, rows_n + 2)

    @pl.when(jnp.logical_not(inner))
    def _():
        pl.semaphore_wait(barrier, rows_n + 1)

    def send(src, dst, s_sem, r_sem, row, col):
        return pltpu.make_async_remote_copy(
            src_ref=src, dst_ref=dst, send_sem=s_sem, recv_sem=r_sem,
            device_id=(row, col), device_id_type=MESH,
        )

    width = g_ref.shape[1]
    relayed = rows_n == 4 and width % 256 == 0
    cut = width // 2 if relayed else width
    halves = (slice(0, cut), slice(cut, width)) if relayed else (slice(0, width),)

    def g_copy(j, k):
        return send(gall.at[0:trow, halves[k]], gall.at[j * trow:(j + 1) * trow, halves[k]],
                    gs.at[j, k], gr.at[j, k], exclusive_or(r, j, rows_n), q)

    def g_relay(j):
        k = j - 1
        return send(gall.at[j * trow:(j + 1) * trow, halves[k]], gall.at[3 * trow:4 * trow, halves[k]],
                    gs.at[3, k], gr.at[3, k], exclusive_or(r, 3 - j, rows_n), q)

    if relayed:
        first = [g_copy(1, 0), g_copy(2, 1), g_copy(1, 1), g_copy(2, 0)]
        second = [g_relay(1), g_relay(2)]
    else:
        first = [g_copy(j, 0) for j in range(1, rows_n)]
        second = []
    for copy in first:
        copy.start()

    def x_rows(chip, core):
        return pl.ds(pl.multiple_of(exclusive_or(r, chip, chips) * (2 * tcol) + core * tcol, tcol), tcol)

    own = xall.at[x_rows(z, c)]
    own_up = send(x_ref, own, xs_up.at[z], xr.at[z], r, up)
    own_dn = send(x_ref, own, xs_dn.at[z], xr.at[z], r, down)
    own_p = send(x_ref, own, xs_p.at[z], xp.at[z], r, mate)

    @pl.when(z < chips - 1)
    def _():
        own_up.start()

    @pl.when(z > 0)
    def _():
        own_dn.start()

    own_p.start()
    xall[x_rows(z, c), :] = x_ref[...]

    def block_copies(chip):
        block = xall.at[x_rows(chip, c)]
        return (send(block, block, xs_up.at[chip], xr.at[chip], r, up),
                send(block, block, xs_dn.at[chip], xr.at[chip], r, down),
                send(block, block, xs_p.at[chip], xp.at[chip], r, mate))

    def forward(distance):
        @pl.when(z >= distance)
        def _():
            to_up, _unused, to_mate = block_copies(z - distance)
            to_up.wait_recv()

            @pl.when(z < chips - 1)
            def _():
                to_up.start()

            to_mate.start()

        @pl.when(z + distance < chips)
        def _():
            _unused, to_dn, to_mate = block_copies(z + distance)
            to_dn.wait_recv()

            @pl.when(z > 0)
            def _():
                to_dn.start()

            to_mate.start()

    def part(h):
        return pl.ds(pl.multiple_of(h * dc, dc), dc)

    def pair_copy(h):
        return send(pb.at[1 - c, :, :, part(h)], rb.at[:, :, part(h)], ps.at[h], pr.at[h], r, mate)

    def pair_sum(b, h):
        j = exclusive_or(r, b, rows_n)
        return pb[c, j, :, part(h)].astype(jnp.float32) + rb[j, :, part(h)].astype(jnp.float32)

    def up_copy(b, h):
        return send(sb_up.at[b, :, part(h)], ub.at[b, :, part(h)], us.at[b, h], ur.at[b, h], r, up)

    def dn_copy(b, h):
        return send(sb_dn.at[b, :, part(h)], db.at[b, :, part(h)], ds.at[b, h], dr.at[b, h], r, down)

    def up_step(h):
        def body(i, carry):
            b = chips - 1 - i
            copy = up_copy(b, h)

            @pl.when(z == 0)
            def _():
                sb_up[b, :, part(h)] = pair_sum(b, h).astype(jnp.bfloat16)

            @pl.when(z > 0)
            def _():
                copy.wait_recv()
                sb_up[b, :, part(h)] = (pair_sum(b, h) + ub[b, :, part(h)].astype(jnp.float32)).astype(jnp.bfloat16)

            copy.start()
            return carry

        lax.fori_loop(0, chips - 1 - z, body, 0)

    def dn_step(h):
        def body(b, carry):
            copy = dn_copy(b, h)

            @pl.when(z == chips - 1)
            def _():
                sb_dn[b, :, part(h)] = pair_sum(b, h).astype(jnp.bfloat16)

            @pl.when(z < chips - 1)
            def _():
                copy.wait_recv()
                sb_dn[b, :, part(h)] = (pair_sum(b, h) + db[b, :, part(h)].astype(jnp.float32)).astype(jnp.bfloat16)

            copy.start()
            return carry

        lax.fori_loop(0, z, body, 0)

    def final_step(h):
        total = pair_sum(z, h)

        @pl.when(z > 0)
        def _():
            up_copy(z, h).wait_recv()

        @pl.when(z < chips - 1)
        def _():
            dn_copy(z, h).wait_recv()

        @pl.when(z == 0)
        def _():
            out_ref[:, part(h)] = (total + db[z, :, part(h)].astype(jnp.float32)).astype(jnp.bfloat16)

        @pl.when(z == chips - 1)
        def _():
            out_ref[:, part(h)] = (total + ub[z, :, part(h)].astype(jnp.float32)).astype(jnp.bfloat16)

        @pl.when((z > 0) & (z < chips - 1))
        def _():
            out_ref[:, part(h)] = (total + ub[z, :, part(h)].astype(jnp.float32)
                                   + db[z, :, part(h)].astype(jnp.float32)).astype(jnp.bfloat16)

    tile = min(dc, 512)

    def multiply(h):
        w_copy(h).wait()

        def body(t, carry):
            at = pl.multiple_of(h * dc + t * tile, tile)
            product = lax.dot_general(
                w_v[pl.ds(at, tile), :], gall[...], (((1,), (1,)), ((), ())),
                preferred_element_type=jnp.float32,
            )
            flat = product.T.astype(jnp.bfloat16)
            for j in range(rows_n):
                for core in range(2):
                    first = j * trow + core * tcol
                    pb[core, j, :, pl.ds(at, tile)] = flat[first:first + tcol, :]
            return carry

        lax.fori_loop(0, dc // tile, body, 0)
        pair_copy(h).start()

    for copy, relay in zip(first, second):
        copy.wait_recv()
        relay.start()
    forward(1)
    for copy in first[len(second):] + second:
        copy.wait_recv()

    last = PAIR_LAG + LEVEL_LAG * (chips - 1)
    for slot in range(parts + last):
        if slot < parts:
            multiply(slot)
        if 0 <= slot - PAIR_LAG < parts:
            pair_copy(slot - PAIR_LAG).wait_recv()
        h_up = slot - PAIR_LAG - LEVEL_LAG * z
        h_dn = slot - PAIR_LAG - LEVEL_LAG * (chips - 1 - z)

        @pl.when((h_up >= 0) & (h_up < parts))
        def _():
            up_step(h_up)

        @pl.when((h_dn >= 0) & (h_dn < parts))
        def _():
            dn_step(h_dn)

        if 0 <= slot - last < parts:
            final_step(slot - last)
        if slot == parts // 4:
            for distance in range(2, chips - 1):
                forward(distance)
    if chips > 2:
        forward(chips - 1)

    for copy in first + second:
        copy.wait_send()
    for h in range(parts):
        pair_copy(h).wait_send()
    for chip in range(chips):
        to_up, to_dn, to_mate = block_copies(chip)
        to_mate.wait()

        @pl.when((z >= chip) & (z < chips - 1))
        def _():
            to_up.wait_send()

        @pl.when((z <= chip) & (z > 0))
        def _():
            to_dn.wait_send()

        for h in range(parts):
            @pl.when(z < chip)
            def _():
                up_copy(chip, h).wait_send()

            @pl.when(z > chip)
            def _():
                dn_copy(chip, h).wait_send()


def staged_kernel(rows_n, chips, parts, g_hbm, pos_ref, x_hbm, w_ref, gall, xall, own_ref, up_ref, dn_ref,
                  w_v, raw, pb, rb, ub, db, sb_up, sb_dn,
                  w_sem, in_sem, gs, gr, xs_up, xs_dn, xs_p, xr, xp, ps, pr, us, ur, ds, dr):
    r = lax.axis_index("row")
    q = lax.axis_index("col")
    z, c = q // 2, q % 2
    mate = z * 2 + 1 - c
    up, down = q + 2, q - 2
    trow, width = g_hbm.shape
    tcol, depth = x_hbm.shape
    dc = depth // parts
    pieces = 2
    prow = tcol // pieces

    def x_rows(chip, core, p):
        first = exclusive_or(r, chip, chips) * (2 * tcol) + core * tcol + p * prow
        return pl.ds(pl.multiple_of(first, prow), prow)

    g_in = pltpu.make_async_copy(g_hbm, raw, in_sem.at[0])
    g_in.start()
    x_in = [pltpu.make_async_copy(x_hbm.at[pl.ds(p * prow, prow)], xall.at[x_rows(z, c, p)], in_sem.at[1 + p])
            for p in range(pieces)]
    for copy in x_in:
        copy.start()

    barrier = pltpu.get_barrier_semaphore()
    for j in (1, 2):
        pl.semaphore_signal(barrier, inc=1, device_id=(exclusive_or(r, j, rows_n), q), device_id_type=MESH)
    pl.semaphore_signal(barrier, inc=1, device_id=(r, mate), device_id_type=MESH)

    @pl.when(z > 0)
    def _():
        pl.semaphore_signal(barrier, inc=1, device_id=(r, down), device_id_type=MESH)

    @pl.when(z < chips - 1)
    def _():
        pl.semaphore_signal(barrier, inc=1, device_id=(r, up), device_id_type=MESH)

    def w_copy(h):
        rows = pl.ds(pl.multiple_of(h * dc, dc), dc)
        return pltpu.make_async_copy(w_ref.at[rows], w_v.at[rows], w_sem.at[h])

    for h in range(parts):
        w_copy(h).start()

    g_in.wait()
    unrotate_heads(raw, pos_ref, gall, q * width)
    for copy in x_in:
        copy.wait()

    inner = (z > 0) & (z < chips - 1)

    @pl.when(inner)
    def _():
        pl.semaphore_wait(barrier, 5)

    @pl.when(jnp.logical_not(inner))
    def _():
        pl.semaphore_wait(barrier, 4)

    def send(src, dst, s_sem, r_sem, row, col):
        return pltpu.make_async_remote_copy(
            src_ref=src, dst_ref=dst, send_sem=s_sem, recv_sem=r_sem,
            device_id=(row, col), device_id_type=MESH,
        )

    cut = width // 2
    halves = (slice(0, cut), slice(cut, width))

    def g_copy(j, k):
        return send(gall.at[0:trow, halves[k]], gall.at[j * trow:(j + 1) * trow, halves[k]],
                    gs.at[j, k], gr.at[j, k], exclusive_or(r, j, rows_n), q)

    def g_relay(j):
        k = j - 1
        return send(gall.at[j * trow:(j + 1) * trow, halves[k]], gall.at[3 * trow:4 * trow, halves[k]],
                    gs.at[3, k], gr.at[3, k], exclusive_or(r, 3 - j, rows_n), q)

    g_first = [g_copy(1, 0), g_copy(2, 1)]
    g_second = [g_copy(1, 1), g_copy(2, 0)]
    g_third = [g_relay(1), g_relay(2)]
    for copy in g_first + g_second:
        copy.start()

    def block_copies(chip, p):
        block = xall.at[x_rows(chip, c, p)]
        return (send(block, block, xs_up.at[chip, p], xr.at[chip, p], r, up),
                send(block, block, xs_dn.at[chip, p], xr.at[chip, p], r, down),
                send(block, block, xs_p.at[chip, p], xp.at[chip, p], r, mate))

    for p in range(pieces):
        to_up, to_dn, to_mate = block_copies(z, p)

        @pl.when(z < chips - 1)
        def _():
            to_up.start()

        @pl.when(z > 0)
        def _():
            to_dn.start()

        to_mate.start()

    def forward(distance, p):
        @pl.when(z >= distance)
        def _():
            to_up, _unused, to_mate = block_copies(z - distance, p)
            to_up.wait_recv()

            @pl.when(z < chips - 1)
            def _():
                to_up.start()

            to_mate.start()

        @pl.when(z + distance < chips)
        def _():
            _unused, to_dn, to_mate = block_copies(z + distance, p)
            to_dn.wait_recv()

            @pl.when(z > 0)
            def _():
                to_dn.start()

            to_mate.start()

    def part(h):
        return pl.ds(pl.multiple_of(h * dc, dc), dc)

    def pair_copy(j, h):
        return send(pb.at[1 - c, j, :, part(h)], rb.at[j, :, part(h)], ps.at[j, h], pr.at[j, h], r, mate)

    def pair_sum(j, h):
        return pb[c, j, :, part(h)].astype(jnp.float32) + rb[j, :, part(h)].astype(jnp.float32)

    def up_copy(j, h):
        return send(sb_up.at[j, :, part(h)], ub.at[j, :, part(h)], us.at[j, h], ur.at[j, h], r, up)

    def dn_copy(j, h):
        return send(sb_dn.at[j, :, part(h)], db.at[j, :, part(h)], ds.at[j, h], dr.at[j, h], r, down)

    def multiply(i, first, last):
        h = i % parts
        product = lax.dot_general(
            w_v[part(h), :], gall[first * trow:last * trow, :], (((1,), (1,)), ((), ())),
            preferred_element_type=jnp.float32,
        )
        flat = product.T.astype(half)
        for j in range(first, last):
            for core in range(2):
                at = (j - first) * trow + core * tcol
                pb[core, j, :, part(h)] = flat[at:at + tcol, :]
        for j in range(first, last):
            pair_copy(j, h).start()

    def each_block(i, act):
        def body(j, carry):
            least = parts * ((j + 3) // 4) + (parts // 2) * (j // 3)

            @pl.when((i >= least) & (i < least + parts))
            def _():
                act(j, (i + 4 * LEVEL_LAG * parts) % parts, exclusive_or(r, j, rows_n))

            return carry

        lax.fori_loop(0, rows_n, body, 0)

    def own_step(j, h, dest):
        pair_copy(j, h).wait_recv()

        @pl.when(dest == z)
        def _():
            own_ref[:, part(h)] = pair_sum(j, h)

    def up_step(j, h, dest):
        copy = up_copy(j, h)

        def finish(total):
            @pl.when(dest == z + 1)
            def _():
                up_ref[:, part(h)] = total.astype(half)

            @pl.when(dest > z + 1)
            def _():
                sb_up[j, :, part(h)] = total.astype(half)
                copy.start()

        @pl.when((dest > z) & (z == 0))
        def _():
            finish(pair_sum(j, h))

        @pl.when((dest > z) & (z > 0))
        def _():
            copy.wait_recv()
            finish(pair_sum(j, h) + ub[j, :, part(h)].astype(jnp.float32))

    def dn_step(j, h, dest):
        copy = dn_copy(j, h)

        def finish(total):
            @pl.when(dest == z - 1)
            def _():
                dn_ref[:, part(h)] = total.astype(half)

            @pl.when(dest < z - 1)
            def _():
                sb_dn[j, :, part(h)] = total.astype(half)
                copy.start()

        @pl.when((dest < z) & (z == chips - 1))
        def _():
            finish(pair_sum(j, h))

        @pl.when((dest < z) & (z < chips - 1))
        def _():
            copy.wait_recv()
            finish(pair_sum(j, h) + db[j, :, part(h)].astype(jnp.float32))

    def settle(slot):
        each_block(slot - 1, own_step)
        each_block(slot - 1 - LEVEL_LAG * z, up_step)
        each_block(slot - 1 - LEVEL_LAG * (chips - 1 - z), dn_step)

    def products(start, stop, first, last, after):
        def body(i, carry):
            if start == 0:
                w_copy(i).wait()
            multiply(i, first, last)
            for at, act in after:
                pl.when(i == at)(act)
            settle(i)
            return carry

        lax.fori_loop(start, stop, body, 0)

    def early():
        for copy, relay in zip(g_first, g_third):
            copy.wait_recv()
            relay.start()
        forward(1, 0)

    half_way = parts // 2
    products(0, parts, 0, 1, [(parts - 2, early), (parts - 1, lambda: forward(1, 1))])
    for copy in g_second:
        copy.wait_recv()
    products(parts, parts + half_way, 1, 3, [(parts + half_way - 1, lambda: forward(2, 0))])
    for copy in g_third:
        copy.wait_recv()
    products(parts + half_way, 2 * parts, 1, 4, [(parts + half_way, lambda: forward(2, 1))])
    products(2 * parts, 2 * parts + half_way, 3, 4, [(2 * parts, lambda: forward(3, 0))])

    @pl.when(z == 0)
    def _():
        dn_ref[...] = jnp.zeros_like(dn_ref)

    @pl.when(z == chips - 1)
    def _():
        up_ref[...] = jnp.zeros_like(up_ref)

    def drain(slot, carry):
        settle(slot)
        return carry

    first_slot = 2 * parts + half_way
    lax.fori_loop(first_slot, first_slot + LEVEL_LAG, drain, 0)
    forward(3, 1)
    lax.fori_loop(first_slot + LEVEL_LAG, first_slot + 1 + LEVEL_LAG * (chips - 2), drain, 0)

    for copy in g_first + g_second + g_third:
        copy.wait_send()
    for chip in range(chips):
        for p in range(pieces):
            to_up, to_dn, to_mate = block_copies(chip, p)
            to_mate.wait()

            @pl.when((z >= chip) & (z < chips - 1))
            def _():
                to_up.wait_send()

            @pl.when((z <= chip) & (z > 0))
            def _():
                to_dn.wait_send()

    def sent(j, carry):
        dest = exclusive_or(r, j, rows_n)
        for h in range(parts):
            pair_copy(j, h).wait_send()

            @pl.when(dest > z + 1)
            def _():
                up_copy(j, h).wait_send()

            @pl.when(dest < z - 1)
            def _():
                dn_copy(j, h).wait_send()
        return carry

    lax.fori_loop(0, rows_n, sent, 0)


def outer_kernel(x_ref, g_ref, out_ref, buf, sem):
    slots, block, _ = buf.shape
    steps = out_ref.shape[0] // block

    def rows(i):
        return pl.ds(pl.multiple_of(i * block, block), block)

    def out_copy(i):
        slot = lax.rem(i, slots)
        return pltpu.make_async_copy(buf.at[slot], out_ref.at[rows(i)], sem.at[slot])

    def body(i, carry):
        @pl.when(i >= slots)
        def _():
            out_copy(i - slots).wait()

        buf[lax.rem(i, slots), :, :] = lax.dot_general(
            x_ref[:, rows(i)], g_ref[...], (((0,), (0,)), ((), ())), preferred_element_type=jnp.float32
        )
        out_copy(i).start()
        return carry

    lax.fori_loop(0, steps, body, 0)
    for i in range(steps - slots, steps):
        out_copy(i).wait()


def outer_streamed(left, right):
    tokens, depth = left.shape
    width = right.shape[1]
    block, slots = 2 * HEAD, 4
    vmem = pl.BlockSpec(memory_space=pltpu.VMEM)
    return pl.pallas_call(
        outer_kernel,
        out_shape=jax.ShapeDtypeStruct((depth, width), jnp.float32),
        in_specs=[vmem, vmem],
        out_specs=pl.BlockSpec(memory_space=pltpu.HBM),
        scratch_shapes=[pltpu.VMEM((slots, block, width), jnp.float32), pltpu.SemaphoreType.DMA((slots,))],
        compiler_params=pltpu.CompilerParams(vmem_limit_bytes=24 * 2**20),
        cost_estimate=pl.CostEstimate(
            flops=2 * tokens * depth * width, bytes_accessed=4 * depth * width, transcendentals=0
        ),
    )(left, right)


def staged(rows_n, chips, inputs, weight, grad_out, positions):
    depth, width = weight.shape
    trow, tcol = grad_out.shape[0], inputs.shape[0]
    parts = 4
    dma = pltpu.SemaphoreType.DMA
    vmem = pl.BlockSpec(memory_space=pltpu.VMEM)
    hbm = pl.BlockSpec(memory_space=pltpu.HBM)
    whole_grad, whole_inputs, own, upward, downward = pl.pallas_call(
        functools.partial(staged_kernel, rows_n, chips, parts),
        out_shape=(
            jax.ShapeDtypeStruct((rows_n * trow, width), half),
            jax.ShapeDtypeStruct((chips * 2 * tcol, depth), half),
            jax.ShapeDtypeStruct((tcol, depth), jnp.float32),
            jax.ShapeDtypeStruct((tcol, depth), half),
            jax.ShapeDtypeStruct((tcol, depth), half),
        ),
        in_specs=[hbm, vmem, hbm, hbm],
        out_specs=(vmem,) * 5,
        scratch_shapes=[
            pltpu.VMEM((depth, width), half),
            pltpu.VMEM((trow, width), half),
            pltpu.VMEM((2, rows_n, tcol, depth), half),
            pltpu.VMEM((rows_n, tcol, depth), half),
            pltpu.VMEM((rows_n, tcol, depth), half),
            pltpu.VMEM((rows_n, tcol, depth), half),
            pltpu.VMEM((rows_n, tcol, depth), half),
            pltpu.VMEM((rows_n, tcol, depth), half),
            dma((parts,)), dma((3,)),
            dma((rows_n, 2)), dma((rows_n, 2)),
            dma((chips, 2)), dma((chips, 2)), dma((chips, 2)), dma((chips, 2)), dma((chips, 2)),
            dma((rows_n, parts)), dma((rows_n, parts)),
            dma((rows_n, parts)), dma((rows_n, parts)), dma((rows_n, parts)), dma((rows_n, parts)),
        ],
        compiler_params=pltpu.CompilerParams(
            collective_id=0, has_side_effects=True, vmem_limit_bytes=44 * 2**20
        ),
        cost_estimate=pl.CostEstimate(
            flops=2 * rows_n * trow * width * depth, bytes_accessed=2 * width * depth, transcendentals=0
        ),
    )(grad_out, positions[None, :], inputs, weight)
    cols = 2 * chips
    from_below = lax.ppermute(upward, "col", [(q, q + 2) for q in range(cols - 2)])
    from_above = lax.ppermute(downward, "col", [(q + 2, q) for q in range(cols - 2)])
    weight_grad = outer_streamed(whole_inputs, whole_grad)
    input_grad = (own + from_below.astype(jnp.float32) + from_above.astype(jnp.float32)).astype(half)
    return (input_grad, weight_grad)


def outer_sum(left, right):
    return lax.dot_general(
        left, right, (((0,), (0,)), ((), ())), preferred_element_type=jnp.float32
    )


def per_device(rows_n, chips, inputs, weight, grad_out, positions):
    depth, width = weight.shape
    trow, tcol = grad_out.shape[0], inputs.shape[0]
    if rows_n == 4 and chips == 4 and width % (2 * HEAD) == 0 and depth % (8 * HEAD) == 0 and trow == 2 * tcol:
        return staged(rows_n, chips, inputs, weight, grad_out, positions)
    col_start = lax.axis_index("col") * width
    raw = width % HEAD == 0
    grad = grad_out if raw else unrotate(grad_out, positions, col_start)
    parts = 8 if depth % (8 * HEAD) == 0 else 4
    dma = pltpu.SemaphoreType.DMA
    vmem = pl.BlockSpec(memory_space=pltpu.VMEM)
    whole_grad, whole_inputs, input_grad = pl.pallas_call(
        functools.partial(kernel, rows_n, chips, parts, raw),
        out_shape=(
            jax.ShapeDtypeStruct((rows_n * trow, width), half),
            jax.ShapeDtypeStruct((chips * 2 * tcol, depth), half),
            jax.ShapeDtypeStruct((tcol, depth), half),
        ),
        in_specs=[vmem, vmem, vmem, pl.BlockSpec(memory_space=pl.ANY)],
        out_specs=(vmem, vmem, vmem),
        scratch_shapes=[
            pltpu.VMEM((depth, width), half),
            pltpu.VMEM((2, rows_n, tcol, depth), half),
            pltpu.VMEM((rows_n, tcol, depth), half),
            pltpu.VMEM((chips, tcol, depth), half),
            pltpu.VMEM((chips, tcol, depth), half),
            pltpu.VMEM((chips, tcol, depth), half),
            pltpu.VMEM((chips, tcol, depth), half),
            dma((parts,)),
            dma((rows_n, 2)), dma((rows_n, 2)),
            dma((chips,)), dma((chips,)), dma((chips,)), dma((chips,)), dma((chips,)),
            dma((parts,)), dma((parts,)),
            dma((chips, parts)), dma((chips, parts)), dma((chips, parts)), dma((chips, parts)),
        ],
        compiler_params=pltpu.CompilerParams(
            collective_id=0, has_side_effects=True, vmem_limit_bytes=60 * 2**20
        ),
        cost_estimate=pl.CostEstimate(
            flops=2 * rows_n * trow * width * depth, bytes_accessed=2 * width * depth, transcendentals=0
        ),
    )(grad, positions[None, :], inputs, weight)
    weight_grad = outer_sum(whole_inputs, whole_grad)
    return (input_grad, weight_grad)


def solution(mesh):
    rows_n, chips = mesh.shape["row"], mesh.shape["col"] // 2
    in_specs = (P("col", "row"), P("row", "col"), P("row", "col"), P("row"))
    out_specs = (P("col", "row"), P("row", "col"))
    return jax.shard_map(
        functools.partial(per_device, rows_n, chips), mesh=mesh, in_specs=in_specs,
        out_specs=out_specs, check_vma=False,
    )
```

```python
import functools
import math

import jax
import jax.numpy as jnp
from jax import lax
from jax.experimental import pallas as pl
from jax.experimental.pallas import tpu as pltpu
from jax.sharding import PartitionSpec as P

QHEADS = 128
KVHEADS = 8
HEAD = 128
PAIR_LAG = 2
LEVEL_LAG = 3
CHAIN_LAG = 3
MESH = pl.DeviceIdType.MESH
half = jnp.bfloat16


def scaled_freq(within):
    base = jnp.exp(-(2.0 * within.astype(jnp.float32) / HEAD) * math.log(500000.0))
    wave = 2.0 * math.pi / base
    smooth = (8192.0 / wave - 1.0) / 3.0
    middle = (1.0 - smooth) * base / 8.0 + smooth * base
    return jnp.where(wave < 2048.0, base, jnp.where(wave > 8192.0, base / 8.0, middle))


def unrotate(grad, positions, col_start):
    width = grad.shape[1]
    lanes = col_start + jnp.arange(HEAD, dtype=jnp.int32)
    freq = scaled_freq(lanes % HEAD // 2)
    angle = positions.astype(jnp.float32)[:, None] * freq[None, :]
    cosine = jnp.cos(angle)
    sine = jnp.where((lanes % 2 == 0)[None, :], jnp.sin(angle), -jnp.sin(angle))
    reps = -(-width // HEAD)
    cosine = jnp.tile(cosine, (1, reps))[:, :width]
    sine = jnp.tile(sine, (1, reps))[:, :width]
    columns = col_start + jnp.arange(width, dtype=jnp.int32)
    rotated = (columns < (QHEADS + KVHEADS) * HEAD)[None, :]
    wide = grad.astype(jnp.float32)
    other = jnp.where(
        (columns % 2 == 0)[None, :], jnp.roll(wide, -1, axis=1), jnp.roll(wide, 1, axis=1)
    )
    return jnp.where(rotated, wide * cosine + other * sine, wide).astype(jnp.bfloat16)


def unrotate_heads(g_ref, pos_ref, out, col_start):
    trow, width = g_ref.shape
    lanes = col_start + lax.broadcasted_iota(jnp.int32, (trow, HEAD), 1)
    freq = scaled_freq((col_start + lax.broadcasted_iota(jnp.int32, (8, HEAD), 1)) % HEAD // 2)[0:1, :]
    row = lax.broadcasted_iota(jnp.int32, (trow, trow), 0)
    lane = lax.broadcasted_iota(jnp.int32, (trow, trow), 1)
    spread = jnp.broadcast_to(pos_ref[...].astype(jnp.float32), (trow, trow))
    column = jnp.sum(jnp.where(row == lane, spread, 0.0), axis=1, keepdims=True)
    angle = column * freq
    even = lanes % 2 == 0
    cosine = jnp.cos(angle)
    sine = jnp.sin(angle)
    sine = jnp.where(even, sine, -sine)
    for first in range(0, width, HEAD):
        wide = g_ref[:, first:first + HEAD].astype(jnp.float32)
        other = jnp.where(even, pltpu.roll(wide, HEAD - 1, 1), pltpu.roll(wide, 1, 1))
        turned = wide * cosine + other * sine
        rotated = lanes + first < (QHEADS + KVHEADS) * HEAD
        out[0:trow, first:first + HEAD] = jnp.where(rotated, turned, wide).astype(jnp.bfloat16)


def exclusive_or(a, b, size):
    total, bit = 0, 1
    while bit < size:
        total = total + bit * ((a // bit % 2 + b // bit % 2) % 2)
        bit *= 2
    return total


def kernel(rows_n, chips, parts, raw, g_ref, pos_ref, x_ref, w_ref, gall, xall, out_ref,
           w_v, pb, rb, ub, db, sb_up, sb_dn,
           w_sem, gs, gr, xs_up, xs_dn, xs_p, xr, xp, ps, pr, us, ur, ds, dr):
    r = lax.axis_index("row")
    q = lax.axis_index("col")
    z, c = q // 2, q % 2
    mate = z * 2 + 1 - c
    up, down = q + 2, q - 2
    trow, tcol = g_ref.shape[0], x_ref.shape[0]
    depth = w_ref.shape[0]
    dc = depth // parts

    def w_copy(h):
        rows = pl.ds(h * dc, dc)
        return pltpu.make_async_copy(w_ref.at[rows], w_v.at[rows], w_sem.at[h])

    for h in range(parts):
        w_copy(h).start()

    if raw:
        unrotate_heads(g_ref, pos_ref, gall, q * g_ref.shape[1])
    else:
        gall[0:trow, :] = g_ref[...]

    barrier = pltpu.get_barrier_semaphore()
    for j in range(1, rows_n):
        pl.semaphore_signal(barrier, inc=1, device_id=(exclusive_or(r, j, rows_n), q), device_id_type=MESH)
    pl.semaphore_signal(barrier, inc=1, device_id=(r, mate), device_id_type=MESH)

    @pl.when(z > 0)
    def _():
        pl.semaphore_signal(barrier, inc=1, device_id=(r, down), device_id_type=MESH)

    @pl.when(z < chips - 1)
    def _():
        pl.semaphore_signal(barrier, inc=1, device_id=(r, up), device_id_type=MESH)

    inner = (z > 0) & (z < chips - 1)

    @pl.when(inner)
    def _():
        pl.semaphore_wait(barrier, rows_n + 2)

    @pl.when(jnp.logical_not(inner))
    def _():
        pl.semaphore_wait(barrier, rows_n + 1)

    def send(src, dst, s_sem, r_sem, row, col):
        return pltpu.make_async_remote_copy(
            src_ref=src, dst_ref=dst, send_sem=s_sem, recv_sem=r_sem,
            device_id=(row, col), device_id_type=MESH,
        )

    width = g_ref.shape[1]
    relayed = rows_n == 4 and width % 256 == 0
    cut = width // 2 if relayed else width
    halves = (slice(0, cut), slice(cut, width)) if relayed else (slice(0, width),)

    def g_copy(j, k):
        return send(gall.at[0:trow, halves[k]], gall.at[j * trow:(j + 1) * trow, halves[k]],
                    gs.at[j, k], gr.at[j, k], exclusive_or(r, j, rows_n), q)

    def g_relay(j):
        k = j - 1
        return send(gall.at[j * trow:(j + 1) * trow, halves[k]], gall.at[3 * trow:4 * trow, halves[k]],
                    gs.at[3, k], gr.at[3, k], exclusive_or(r, 3 - j, rows_n), q)

    if relayed:
        first = [g_copy(1, 0), g_copy(2, 1), g_copy(1, 1), g_copy(2, 0)]
        second = [g_relay(1), g_relay(2)]
    else:
        first = [g_copy(j, 0) for j in range(1, rows_n)]
        second = []
    for copy in first:
        copy.start()

    def x_rows(chip, core):
        return pl.ds(pl.multiple_of(exclusive_or(r, chip, chips) * (2 * tcol) + core * tcol, tcol), tcol)

    own = xall.at[x_rows(z, c)]
    own_up = send(x_ref, own, xs_up.at[z], xr.at[z], r, up)
    own_dn = send(x_ref, own, xs_dn.at[z], xr.at[z], r, down)
    own_p = send(x_ref, own, xs_p.at[z], xp.at[z], r, mate)

    @pl.when(z < chips - 1)
    def _():
        own_up.start()

    @pl.when(z > 0)
    def _():
        own_dn.start()

    own_p.start()
    xall[x_rows(z, c), :] = x_ref[...]

    def block_copies(chip):
        block = xall.at[x_rows(chip, c)]
        return (send(block, block, xs_up.at[chip], xr.at[chip], r, up),
                send(block, block, xs_dn.at[chip], xr.at[chip], r, down),
                send(block, block, xs_p.at[chip], xp.at[chip], r, mate))

    def forward(distance):
        @pl.when(z >= distance)
        def _():
            to_up, _unused, to_mate = block_copies(z - distance)
            to_up.wait_recv()

            @pl.when(z < chips - 1)
            def _():
                to_up.start()

            to_mate.start()

        @pl.when(z + distance < chips)
        def _():
            _unused, to_dn, to_mate = block_copies(z + distance)
            to_dn.wait_recv()

            @pl.when(z > 0)
            def _():
                to_dn.start()

            to_mate.start()

    def part(h):
        return pl.ds(pl.multiple_of(h * dc, dc), dc)

    def pair_copy(h):
        return send(pb.at[1 - c, :, :, part(h)], rb.at[:, :, part(h)], ps.at[h], pr.at[h], r, mate)

    def pair_sum(b, h):
        j = exclusive_or(r, b, rows_n)
        return pb[c, j, :, part(h)].astype(jnp.float32) + rb[j, :, part(h)].astype(jnp.float32)

    def up_copy(b, h):
        return send(sb_up.at[b, :, part(h)], ub.at[b, :, part(h)], us.at[b, h], ur.at[b, h], r, up)

    def dn_copy(b, h):
        return send(sb_dn.at[b, :, part(h)], db.at[b, :, part(h)], ds.at[b, h], dr.at[b, h], r, down)

    def up_step(h):
        def body(i, carry):
            b = chips - 1 - i
            copy = up_copy(b, h)

            @pl.when(z == 0)
            def _():
                sb_up[b, :, part(h)] = pair_sum(b, h).astype(jnp.bfloat16)

            @pl.when(z > 0)
            def _():
                copy.wait_recv()
                sb_up[b, :, part(h)] = (pair_sum(b, h) + ub[b, :, part(h)].astype(jnp.float32)).astype(jnp.bfloat16)

            copy.start()
            return carry

        lax.fori_loop(0, chips - 1 - z, body, 0)

    def dn_step(h):
        def body(b, carry):
            copy = dn_copy(b, h)

            @pl.when(z == chips - 1)
            def _():
                sb_dn[b, :, part(h)] = pair_sum(b, h).astype(jnp.bfloat16)

            @pl.when(z < chips - 1)
            def _():
                copy.wait_recv()
                sb_dn[b, :, part(h)] = (pair_sum(b, h) + db[b, :, part(h)].astype(jnp.float32)).astype(jnp.bfloat16)

            copy.start()
            return carry

        lax.fori_loop(0, z, body, 0)

    def final_step(h):
        total = pair_sum(z, h)

        @pl.when(z > 0)
        def _():
            up_copy(z, h).wait_recv()

        @pl.when(z < chips - 1)
        def _():
            dn_copy(z, h).wait_recv()

        @pl.when(z == 0)
        def _():
            out_ref[:, part(h)] = (total + db[z, :, part(h)].astype(jnp.float32)).astype(jnp.bfloat16)

        @pl.when(z == chips - 1)
        def _():
            out_ref[:, part(h)] = (total + ub[z, :, part(h)].astype(jnp.float32)).astype(jnp.bfloat16)

        @pl.when((z > 0) & (z < chips - 1))
        def _():
            out_ref[:, part(h)] = (total + ub[z, :, part(h)].astype(jnp.float32)
                                   + db[z, :, part(h)].astype(jnp.float32)).astype(jnp.bfloat16)

    tile = min(dc, 512)

    def multiply(h):
        w_copy(h).wait()

        def body(t, carry):
            at = pl.multiple_of(h * dc + t * tile, tile)
            product = lax.dot_general(
                w_v[pl.ds(at, tile), :], gall[...], (((1,), (1,)), ((), ())),
                preferred_element_type=jnp.float32,
            )
            flat = product.T.astype(jnp.bfloat16)
            for j in range(rows_n):
                for core in range(2):
                    first = j * trow + core * tcol
                    pb[core, j, :, pl.ds(at, tile)] = flat[first:first + tcol, :]
            return carry

        lax.fori_loop(0, dc // tile, body, 0)
        pair_copy(h).start()

    for copy, relay in zip(first, second):
        copy.wait_recv()
        relay.start()
    forward(1)
    for copy in first[len(second):] + second:
        copy.wait_recv()

    last = PAIR_LAG + LEVEL_LAG * (chips - 1)
    for slot in range(parts + last):
        if slot < parts:
            multiply(slot)
        if 0 <= slot - PAIR_LAG < parts:
            pair_copy(slot - PAIR_LAG).wait_recv()
        h_up = slot - PAIR_LAG - LEVEL_LAG * z
        h_dn = slot - PAIR_LAG - LEVEL_LAG * (chips - 1 - z)

        @pl.when((h_up >= 0) & (h_up < parts))
        def _():
            up_step(h_up)

        @pl.when((h_dn >= 0) & (h_dn < parts))
        def _():
            dn_step(h_dn)

        if 0 <= slot - last < parts:
            final_step(slot - last)
        if slot == parts // 4:
            for distance in range(2, chips - 1):
                forward(distance)
    if chips > 2:
        forward(chips - 1)

    for copy in first + second:
        copy.wait_send()
    for h in range(parts):
        pair_copy(h).wait_send()
    for chip in range(chips):
        to_up, to_dn, to_mate = block_copies(chip)
        to_mate.wait()

        @pl.when((z >= chip) & (z < chips - 1))
        def _():
            to_up.wait_send()

        @pl.when((z <= chip) & (z > 0))
        def _():
            to_dn.wait_send()

        for h in range(parts):
            @pl.when(z < chip)
            def _():
                up_copy(chip, h).wait_send()

            @pl.when(z > chip)
            def _():
                dn_copy(chip, h).wait_send()


def is_rising(row):
    return row // 2 % 2 == 0


def staged_kernel(rows_n, chips, parts, g_hbm, pos_hbm, x_hbm, w_ref, gall, xall, own_ref, last_ref,
                  w_v, raw, pos_ref, pb, rb, ub, db, sb_up, sb_dn,
                  w_sem, in_sem, gs, gr, xs_up, xs_dn, xs_p, xr, xp, ps, pr, us, ur, ds, dr):
    r = lax.axis_index("row")
    q = lax.axis_index("col")
    z, c = q // 2, q % 2
    mate = z * 2 + 1 - c
    up, down = q + 2, q - 2
    rising = is_rising(r)
    falling = jnp.logical_not(rising)
    trow, width = g_hbm.shape
    tcol, depth = x_hbm.shape
    dc = depth // parts
    pieces = 2
    prow = tcol // pieces

    def x_rows(chip, core, p):
        first = exclusive_or(r, chip, chips) * (2 * tcol) + core * tcol + p * prow
        return pl.ds(pl.multiple_of(first, prow), prow)

    g_in = pltpu.make_async_copy(g_hbm, raw, in_sem.at[0])
    g_in.start()
    pos_in = pltpu.make_async_copy(pos_hbm, pos_ref, in_sem.at[3])
    pos_in.start()
    x_in = [pltpu.make_async_copy(x_hbm.at[pl.ds(p * prow, prow)], xall.at[x_rows(z, c, p)], in_sem.at[1 + p])
            for p in range(pieces)]
    for copy in x_in:
        copy.start()

    barrier = pltpu.get_barrier_semaphore()
    for j in (1, 2):
        pl.semaphore_signal(barrier, inc=1, device_id=(exclusive_or(r, j, rows_n), q), device_id_type=MESH)
    pl.semaphore_signal(barrier, inc=1, device_id=(r, mate), device_id_type=MESH)

    @pl.when(z > 0)
    def _():
        pl.semaphore_signal(barrier, inc=1, device_id=(r, down), device_id_type=MESH)

    @pl.when(z < chips - 1)
    def _():
        pl.semaphore_signal(barrier, inc=1, device_id=(r, up), device_id_type=MESH)

    def w_copy(h):
        rows = pl.ds(pl.multiple_of(h * dc, dc), dc)
        return pltpu.make_async_copy(w_ref.at[rows], w_v.at[rows], w_sem.at[h])

    for h in range(parts):
        w_copy(h).start()

    pos_in.wait()
    g_in.wait()
    unrotate_heads(raw, pos_ref, gall, q * width)
    for copy in x_in:
        copy.wait()

    inner = (z > 0) & (z < chips - 1)

    @pl.when(inner)
    def _():
        pl.semaphore_wait(barrier, 5)

    @pl.when(jnp.logical_not(inner))
    def _():
        pl.semaphore_wait(barrier, 4)

    def send(src, dst, s_sem, r_sem, row, col):
        return pltpu.make_async_remote_copy(
            src_ref=src, dst_ref=dst, send_sem=s_sem, recv_sem=r_sem,
            device_id=(row, col), device_id_type=MESH,
        )

    cut = width // 2
    halves = (slice(0, cut), slice(cut, width))

    def g_copy(j, k):
        return send(gall.at[0:trow, halves[k]], gall.at[j * trow:(j + 1) * trow, halves[k]],
                    gs.at[j, k], gr.at[j, k], exclusive_or(r, j, rows_n), q)

    def g_relay(j):
        k = j - 1
        return send(gall.at[j * trow:(j + 1) * trow, halves[k]], gall.at[3 * trow:4 * trow, halves[k]],
                    gs.at[3, k], gr.at[3, k], exclusive_or(r, 3 - j, rows_n), q)

    g_first = [g_copy(1, 0), g_copy(2, 1)]
    g_second = [g_copy(1, 1), g_copy(2, 0)]
    g_third = [g_relay(1), g_relay(2)]
    for copy in g_first + g_second:
        copy.start()

    def block_copies(chip, p):
        block = xall.at[x_rows(chip, c, p)]
        return (send(block, block, xs_up.at[chip, p], xr.at[chip, p], r, up),
                send(block, block, xs_dn.at[chip, p], xr.at[chip, p], r, down),
                send(block, block, xs_p.at[chip, p], xp.at[chip, p], r, mate))

    for p in range(pieces):
        to_up, to_dn, to_mate = block_copies(z, p)

        @pl.when(z < chips - 1)
        def _():
            to_up.start()

        @pl.when(z > 0)
        def _():
            to_dn.start()

        to_mate.start()

    def forward(distance, p):
        @pl.when(z >= distance)
        def _():
            to_up, _unused, to_mate = block_copies(z - distance, p)
            to_up.wait_recv()

            @pl.when(z < chips - 1)
            def _():
                to_up.start()

            to_mate.start()

        @pl.when(z + distance < chips)
        def _():
            _unused, to_dn, to_mate = block_copies(z + distance, p)
            to_dn.wait_recv()

            @pl.when(z > 0)
            def _():
                to_dn.start()

            to_mate.start()

    def part(h):
        return pl.ds(pl.multiple_of(h * dc, dc), dc)

    def pair_copy(j, h):
        return send(pb.at[1 - c, j, :, part(h)], rb.at[j, :, part(h)], ps.at[j, h], pr.at[j, h], r, mate)

    def pair_sum(j, h):
        return pb[c, j, :, part(h)].astype(jnp.float32) + rb[j, :, part(h)].astype(jnp.float32)

    def up_copy(j, h):
        return send(sb_up.at[j, :, part(h)], ub.at[j, :, part(h)], us.at[j, h], ur.at[j, h], r, up)

    def dn_copy(j, h):
        return send(sb_dn.at[j, :, part(h)], db.at[j, :, part(h)], ds.at[j, h], dr.at[j, h], r, down)

    def multiply(i, first, last):
        h = i % parts
        product = lax.dot_general(
            w_v[part(h), :], gall[first * trow:last * trow, :], (((1,), (1,)), ((), ())),
            preferred_element_type=jnp.float32,
        )
        flat = product.T.astype(half)
        for j in range(first, last):
            for core in range(2):
                at = (j - first) * trow + core * tcol
                pb[core, j, :, part(h)] = flat[at:at + tcol, :]
        for j in range(first, last):
            pair_copy(j, h).start()

    count = 2 * parts + parts // 2
    firsts = [parts * ((j + 3) // 4) + (parts // 2) * (j // 3) for j in range(rows_n)]

    def each_block(slot, lo, hi, lag, act, busy=None, late=None):
        def block(j, guard=None):
            least, most = firsts[j], firsts[j] + parts
            if hi - lag <= least or lo - lag >= most:
                return
            dest = exclusive_or(r, j, rows_n)

            def run():
                act(j, (slot - lag) % parts, dest)

            conds = [] if guard is None else [guard(dest)]
            if lo - lag < least or hi - lag > most:
                conds.append((slot - lag >= least) & (slot - lag < most))
            if conds:
                pl.when(functools.reduce(jnp.logical_and, conds))(run)
            else:
                run()

        last_parts = late is not None and hi - lag > count - parts

        if busy is not False:
            block(3, (lambda dest: dest != late) if last_parts else None)
            block(2, (lambda dest: (dest != late) | (slot - lag < count - parts)) if last_parts else None)
        block(1)
        block(0)
        if last_parts:
            block(3, lambda dest: dest == late)

    def own_step(j, h, dest):
        pair_copy(j, h).wait_recv()

    def chain_step(copy, arrived, sent, busy, ends, origin, near, beyond, here, h, j):
        def total():
            return pair_sum(j, h)

        sends, stays = (beyond, near) if busy else (beyond | near, here)

        def settled(value):
            if ends is not True:
                @pl.when(sends)
                def _():
                    sent[j, :, part(h)] = value.astype(half)
                    copy.start()

            if ends is not False:
                @pl.when(stays)
                def _():
                    if busy:
                        last_ref[:, part(h)] = value.astype(half)
                    else:
                        own_ref[:, part(h)] = value

        takes = sends | stays if ends is None else stays if ends else sends

        @pl.when(takes & jnp.logical_not(origin))
        def _():
            copy.wait_recv()
            settled(total() + arrived[j, :, part(h)].astype(jnp.float32))

        @pl.when((takes & origin))
        def _():
            settled(total())

    def up_step(busy, ends, j, h, dest):
        chain_step(up_copy(j, h), ub, sb_up, busy, ends, z == 0, dest == z + 1, dest > z + 1, dest == z, h, j)

    def dn_step(busy, ends, j, h, dest):
        chain_step(dn_copy(j, h), db, sb_dn, busy, ends, z == chips - 1, dest == z - 1, dest < z - 1, dest == z, h, j)

    late_up, late_dn = 2, chips - 3

    def settle_late(chip):
        for busy, late, at, act in ((rising, late_up, chip, up_step), (falling, late_dn, chips - 1 - chip, dn_step)):
            for i in range(count - parts, 2 * parts):
                dest = exclusive_or(r, 2, rows_n)

                @pl.when((z == at) & (dest == late) & busy)
                def _():
                    act(True, None, 2, i % parts, dest)

    def settle_short(chip, products):
        for idle, at, act in ((falling, chip, up_step), (rising, chips - 1 - chip, dn_step)):
            @pl.when((z == at) & idle)
            def _():
                for i in products:
                    for j in (2, 3):
                        if firsts[j] <= i < firsts[j] + parts:
                            act(False, None, j, i % parts, exclusive_or(r, j, rows_n))

    def settle(slot, lo, hi, ends=None):
        if not ends:
            each_block(slot, lo, hi, 1, own_step)
        for chip in range(chips):
            lag_up, lag_dn = 1 + CHAIN_LAG * chip, 1 + CHAIN_LAG * (chips - 1 - chip)
            ups = hi > lag_up and lo < count + lag_up
            dns = hi > lag_dn and lo < count + lag_dn
            if not (ups or dns):
                continue

            @pl.when((z == chip) & rising)
            def _():
                if dns:
                    each_block(slot, lo, hi, lag_dn, functools.partial(dn_step, False, ends), False)
                if ups:
                    each_block(slot, lo, hi, lag_up, functools.partial(up_step, True, ends), True, late_up)

            @pl.when((z == chip) & falling)
            def _():
                if ups:
                    each_block(slot, lo, hi, lag_up, functools.partial(up_step, False, ends), False)
                if dns:
                    each_block(slot, lo, hi, lag_dn, functools.partial(dn_step, True, ends), True, late_dn)

    def products(start, stop, first, last, after):
        def body(i, carry):
            if start == 0:
                w_copy(i).wait()
            multiply(i, first, last)
            for at, act in after:
                pl.when(i == at)(act)
            settle(i, start, stop)
            return carry

        lax.fori_loop(start, stop, body, 0)

    def early():
        for copy, relay in zip(g_first, g_third):
            copy.wait_recv()
            relay.start()
        forward(1, 0)

    half_way = parts // 2
    products(0, parts, 0, 1, [(parts - 2, early), (parts - 1, lambda: forward(1, 1))])
    for copy in g_second:
        copy.wait_recv()
    products(parts, parts + half_way, 1, 3, [(parts + half_way - 1, lambda: forward(2, 0))])
    for copy in g_third:
        copy.wait_recv()
    products(parts + half_way, 2 * parts, 1, 4, [(parts + half_way, lambda: forward(2, 1))])
    products(2 * parts, 2 * parts + half_way, 3, 4, [(2 * parts, lambda: forward(3, 0))])

    @pl.when((rising & (z == chips - 1)) | (falling & (z == 0)))
    def _():
        last_ref[...] = jnp.zeros_like(last_ref)

    settle_short(0, range(parts, count - 1))
    for slot in range(count, count + 1 + CHAIN_LAG * (chips - 1)):
        settle(slot, slot, slot + 1, False)
        if slot == count:
            forward(3, 1)
            settle_short(0, [count - 1])
            settle_late(0)
    for slot in range(count, count + 1 + CHAIN_LAG * (chips - 1)):
        settle(slot, slot, slot + 1, True)
    settle_late(1)
    settle_short(1, range(parts, count))

    for copy in g_first + g_second + g_third:
        copy.wait_send()
    for chip in range(chips):
        for p in range(pieces):
            to_up, to_dn, to_mate = block_copies(chip, p)
            to_mate.wait()

            @pl.when((z >= chip) & (z < chips - 1))
            def _():
                to_up.wait_send()

            @pl.when((z <= chip) & (z > 0))
            def _():
                to_dn.wait_send()

    def sent(j, carry):
        dest = exclusive_or(r, j, rows_n)
        for h in range(parts):
            pair_copy(j, h).wait_send()

            @pl.when((dest > z + 1) | (falling & (dest == z + 1)))
            def _():
                up_copy(j, h).wait_send()

            @pl.when((dest < z - 1) | (rising & (dest == z - 1)))
            def _():
                dn_copy(j, h).wait_send()
        return carry

    lax.fori_loop(0, rows_n, sent, 0)


def outer_kernel(x_ref, g_ref, out_ref, buf, sem):
    slots, block, _ = buf.shape
    steps = out_ref.shape[0] // block

    def rows(i):
        return pl.ds(pl.multiple_of(i * block, block), block)

    def out_copy(i):
        slot = lax.rem(i, slots)
        return pltpu.make_async_copy(buf.at[slot], out_ref.at[rows(i)], sem.at[slot])

    def body(i, carry):
        @pl.when(i >= slots)
        def _():
            out_copy(i - slots).wait()

        buf[lax.rem(i, slots), :, :] = lax.dot_general(
            x_ref[:, rows(i)], g_ref[...], (((0,), (0,)), ((), ())), preferred_element_type=jnp.float32
        )
        out_copy(i).start()
        return carry

    lax.fori_loop(0, steps, body, 0)
    for i in range(steps - slots, steps):
        out_copy(i).wait()


def outer_streamed(left, right):
    tokens, depth = left.shape
    width = right.shape[1]
    block, slots = 2 * HEAD, 4
    vmem = pl.BlockSpec(memory_space=pltpu.VMEM)
    return pl.pallas_call(
        outer_kernel,
        out_shape=jax.ShapeDtypeStruct((depth, width), jnp.float32),
        in_specs=[vmem, vmem],
        out_specs=pl.BlockSpec(memory_space=pltpu.HBM),
        scratch_shapes=[pltpu.VMEM((slots, block, width), jnp.float32), pltpu.SemaphoreType.DMA((slots,))],
        compiler_params=pltpu.CompilerParams(vmem_limit_bytes=24 * 2**20),
        cost_estimate=pl.CostEstimate(
            flops=2 * tokens * depth * width, bytes_accessed=4 * depth * width, transcendentals=0
        ),
    )(left, right)


def staged(rows_n, chips, inputs, weight, grad_out, positions):
    depth, width = weight.shape
    trow, tcol = grad_out.shape[0], inputs.shape[0]
    parts = 4
    dma = pltpu.SemaphoreType.DMA
    vmem = pl.BlockSpec(memory_space=pltpu.VMEM)
    hbm = pl.BlockSpec(memory_space=pltpu.HBM)
    whole_grad, whole_inputs, own, last = pl.pallas_call(
        functools.partial(staged_kernel, rows_n, chips, parts),
        out_shape=(
            jax.ShapeDtypeStruct((rows_n * trow, width), half),
            jax.ShapeDtypeStruct((chips * 2 * tcol, depth), half),
            jax.ShapeDtypeStruct((tcol, depth), jnp.float32),
            jax.ShapeDtypeStruct((tcol, depth), half),
        ),
        in_specs=[hbm] * 4,
        out_specs=(vmem,) * 4,
        scratch_shapes=[
            pltpu.VMEM((depth, width), half),
            pltpu.VMEM((trow, width), half),
            pltpu.VMEM((1, trow), jnp.int32),
            pltpu.VMEM((2, rows_n, tcol, depth), half),
            pltpu.VMEM((rows_n, tcol, depth), half),
            pltpu.VMEM((rows_n, tcol, depth), half),
            pltpu.VMEM((rows_n, tcol, depth), half),
            pltpu.VMEM((rows_n, tcol, depth), half),
            pltpu.VMEM((rows_n, tcol, depth), half),
            dma((parts,)), dma((4,)),
            dma((rows_n, 2)), dma((rows_n, 2)),
            dma((chips, 2)), dma((chips, 2)), dma((chips, 2)), dma((chips, 2)), dma((chips, 2)),
            dma((rows_n, parts)), dma((rows_n, parts)),
            dma((rows_n, parts)), dma((rows_n, parts)), dma((rows_n, parts)), dma((rows_n, parts)),
        ],
        compiler_params=pltpu.CompilerParams(
            collective_id=0, has_side_effects=True, vmem_limit_bytes=44 * 2**20
        ),
        cost_estimate=pl.CostEstimate(
            flops=2 * rows_n * trow * width * depth, bytes_accessed=2 * width * depth, transcendentals=0
        ),
    )(*(pltpu.with_memory_space_constraint(a, pltpu.HBM) for a in (grad_out, positions[None, :], inputs, weight)))
    cols = 2 * chips
    hops = [(row * cols + q, row * cols + q + 2) for row in range(rows_n) for q in range(cols - 2)]
    hops = [(a, b) if is_rising(a // cols) else (b, a) for a, b in hops]
    arrived = lax.ppermute(last, ("row", "col"), hops)
    weight_grad = outer_streamed(whole_inputs, whole_grad)
    input_grad = (own + arrived.astype(jnp.float32)).astype(half)
    return (input_grad, weight_grad)


def outer_sum(left, right):
    return lax.dot_general(
        left, right, (((0,), (0,)), ((), ())), preferred_element_type=jnp.float32
    )


def per_device(rows_n, chips, inputs, weight, grad_out, positions):
    depth, width = weight.shape
    trow, tcol = grad_out.shape[0], inputs.shape[0]
    if rows_n == 4 and chips == 4 and width % (2 * HEAD) == 0 and depth % (8 * HEAD) == 0 and trow == 2 * tcol:
        return staged(rows_n, chips, inputs, weight, grad_out, positions)
    col_start = lax.axis_index("col") * width
    raw = width % HEAD == 0
    grad = grad_out if raw else unrotate(grad_out, positions, col_start)
    parts = 8 if depth % (8 * HEAD) == 0 else 4
    dma = pltpu.SemaphoreType.DMA
    vmem = pl.BlockSpec(memory_space=pltpu.VMEM)
    whole_grad, whole_inputs, input_grad = pl.pallas_call(
        functools.partial(kernel, rows_n, chips, parts, raw),
        out_shape=(
            jax.ShapeDtypeStruct((rows_n * trow, width), half),
            jax.ShapeDtypeStruct((chips * 2 * tcol, depth), half),
            jax.ShapeDtypeStruct((tcol, depth), half),
        ),
        in_specs=[vmem, vmem, vmem, pl.BlockSpec(memory_space=pl.ANY)],
        out_specs=(vmem, vmem, vmem),
        scratch_shapes=[
            pltpu.VMEM((depth, width), half),
            pltpu.VMEM((2, rows_n, tcol, depth), half),
            pltpu.VMEM((rows_n, tcol, depth), half),
            pltpu.VMEM((chips, tcol, depth), half),
            pltpu.VMEM((chips, tcol, depth), half),
            pltpu.VMEM((chips, tcol, depth), half),
            pltpu.VMEM((chips, tcol, depth), half),
            dma((parts,)),
            dma((rows_n, 2)), dma((rows_n, 2)),
            dma((chips,)), dma((chips,)), dma((chips,)), dma((chips,)), dma((chips,)),
            dma((parts,)), dma((parts,)),
            dma((chips, parts)), dma((chips, parts)), dma((chips, parts)), dma((chips, parts)),
        ],
        compiler_params=pltpu.CompilerParams(
            collective_id=0, has_side_effects=True, vmem_limit_bytes=60 * 2**20
        ),
        cost_estimate=pl.CostEstimate(
            flops=2 * rows_n * trow * width * depth, bytes_accessed=2 * width * depth, transcendentals=0
        ),
    )(grad, positions[None, :], inputs, weight)
    weight_grad = outer_sum(whole_inputs, whole_grad)
    return (input_grad, weight_grad)


def solution(mesh):
    rows_n, chips = mesh.shape["row"], mesh.shape["col"] // 2
    in_specs = (P("col", "row"), P("row", "col"), P("row", "col"), P("row"))
    out_specs = (P("col", "row"), P("row", "col"))
    return jax.shard_map(
        functools.partial(per_device, rows_n, chips), mesh=mesh, in_specs=in_specs,
        out_specs=out_specs, check_vma=False,
    )
```

```python
import functools
import math

import jax
import jax.numpy as jnp
from jax import lax
from jax.experimental import pallas as pl
from jax.experimental.pallas import tpu as pltpu
from jax.sharding import PartitionSpec as P

QHEADS = 128
KVHEADS = 8
HEAD = 128
PAIR_LAG = 2
LEVEL_LAG = 3
CHAIN_LAG = 3
NEAR_LAG = 2
MESH = pl.DeviceIdType.MESH
half = jnp.bfloat16


def scaled_freq(within):
    base = jnp.exp(-(2.0 * within.astype(jnp.float32) / HEAD) * math.log(500000.0))
    wave = 2.0 * math.pi / base
    smooth = (8192.0 / wave - 1.0) / 3.0
    middle = (1.0 - smooth) * base / 8.0 + smooth * base
    return jnp.where(wave < 2048.0, base, jnp.where(wave > 8192.0, base / 8.0, middle))


def unrotate(grad, positions, col_start):
    width = grad.shape[1]
    lanes = col_start + jnp.arange(HEAD, dtype=jnp.int32)
    freq = scaled_freq(lanes % HEAD // 2)
    angle = positions.astype(jnp.float32)[:, None] * freq[None, :]
    cosine = jnp.cos(angle)
    sine = jnp.where((lanes % 2 == 0)[None, :], jnp.sin(angle), -jnp.sin(angle))
    reps = -(-width // HEAD)
    cosine = jnp.tile(cosine, (1, reps))[:, :width]
    sine = jnp.tile(sine, (1, reps))[:, :width]
    columns = col_start + jnp.arange(width, dtype=jnp.int32)
    rotated = (columns < (QHEADS + KVHEADS) * HEAD)[None, :]
    wide = grad.astype(jnp.float32)
    other = jnp.where(
        (columns % 2 == 0)[None, :], jnp.roll(wide, -1, axis=1), jnp.roll(wide, 1, axis=1)
    )
    return jnp.where(rotated, wide * cosine + other * sine, wide).astype(jnp.bfloat16)


def unrotate_heads(g_ref, pos_ref, out, col_start):
    trow, width = g_ref.shape
    lanes = col_start + lax.broadcasted_iota(jnp.int32, (trow, HEAD), 1)
    freq = scaled_freq((col_start + lax.broadcasted_iota(jnp.int32, (8, HEAD), 1)) % HEAD // 2)[0:1, :]
    row = lax.broadcasted_iota(jnp.int32, (trow, trow), 0)
    lane = lax.broadcasted_iota(jnp.int32, (trow, trow), 1)
    spread = jnp.broadcast_to(pos_ref[...].astype(jnp.float32), (trow, trow))
    column = jnp.sum(jnp.where(row == lane, spread, 0.0), axis=1, keepdims=True)
    angle = column * freq
    even = lanes % 2 == 0
    cosine = jnp.cos(angle)
    sine = jnp.sin(angle)
    sine = jnp.where(even, sine, -sine)
    for first in range(0, width, HEAD):
        wide = g_ref[:, first:first + HEAD].astype(jnp.float32)
        other = jnp.where(even, pltpu.roll(wide, HEAD - 1, 1), pltpu.roll(wide, 1, 1))
        turned = wide * cosine + other * sine
        rotated = lanes + first < (QHEADS + KVHEADS) * HEAD
        out[0:trow, first:first + HEAD] = jnp.where(rotated, turned, wide).astype(jnp.bfloat16)


def exclusive_or(a, b, size):
    total, bit = 0, 1
    while bit < size:
        total = total + bit * ((a // bit % 2 + b // bit % 2) % 2)
        bit *= 2
    return total


def kernel(rows_n, chips, parts, raw, g_ref, pos_ref, x_ref, w_ref, gall, xall, out_ref,
           w_v, pb, rb, ub, db, sb_up, sb_dn,
           w_sem, gs, gr, xs_up, xs_dn, xs_p, xr, xp, ps, pr, us, ur, ds, dr):
    r = lax.axis_index("row")
    q = lax.axis_index("col")
    z, c = q // 2, q % 2
    mate = z * 2 + 1 - c
    up, down = q + 2, q - 2
    trow, tcol = g_ref.shape[0], x_ref.shape[0]
    depth = w_ref.shape[0]
    dc = depth // parts

    def w_copy(h):
        rows = pl.ds(h * dc, dc)
        return pltpu.make_async_copy(w_ref.at[rows], w_v.at[rows], w_sem.at[h])

    for h in range(parts):
        w_copy(h).start()

    if raw:
        unrotate_heads(g_ref, pos_ref, gall, q * g_ref.shape[1])
    else:
        gall[0:trow, :] = g_ref[...]

    barrier = pltpu.get_barrier_semaphore()
    for j in range(1, rows_n):
        pl.semaphore_signal(barrier, inc=1, device_id=(exclusive_or(r, j, rows_n), q), device_id_type=MESH)
    pl.semaphore_signal(barrier, inc=1, device_id=(r, mate), device_id_type=MESH)

    @pl.when(z > 0)
    def _():
        pl.semaphore_signal(barrier, inc=1, device_id=(r, down), device_id_type=MESH)

    @pl.when(z < chips - 1)
    def _():
        pl.semaphore_signal(barrier, inc=1, device_id=(r, up), device_id_type=MESH)

    inner = (z > 0) & (z < chips - 1)

    @pl.when(inner)
    def _():
        pl.semaphore_wait(barrier, rows_n + 2)

    @pl.when(jnp.logical_not(inner))
    def _():
        pl.semaphore_wait(barrier, rows_n + 1)

    def send(src, dst, s_sem, r_sem, row, col):
        return pltpu.make_async_remote_copy(
            src_ref=src, dst_ref=dst, send_sem=s_sem, recv_sem=r_sem,
            device_id=(row, col), device_id_type=MESH,
        )

    width = g_ref.shape[1]
    relayed = rows_n == 4 and width % 256 == 0
    cut = width // 2 if relayed else width
    halves = (slice(0, cut), slice(cut, width)) if relayed else (slice(0, width),)

    def g_copy(j, k):
        return send(gall.at[0:trow, halves[k]], gall.at[j * trow:(j + 1) * trow, halves[k]],
                    gs.at[j, k], gr.at[j, k], exclusive_or(r, j, rows_n), q)

    def g_relay(j):
        k = j - 1
        return send(gall.at[j * trow:(j + 1) * trow, halves[k]], gall.at[3 * trow:4 * trow, halves[k]],
                    gs.at[3, k], gr.at[3, k], exclusive_or(r, 3 - j, rows_n), q)

    if relayed:
        first = [g_copy(1, 0), g_copy(2, 1), g_copy(1, 1), g_copy(2, 0)]
        second = [g_relay(1), g_relay(2)]
    else:
        first = [g_copy(j, 0) for j in range(1, rows_n)]
        second = []
    for copy in first:
        copy.start()

    def x_rows(chip, core):
        return pl.ds(pl.multiple_of(exclusive_or(r, chip, chips) * (2 * tcol) + core * tcol, tcol), tcol)

    own = xall.at[x_rows(z, c)]
    own_up = send(x_ref, own, xs_up.at[z], xr.at[z], r, up)
    own_dn = send(x_ref, own, xs_dn.at[z], xr.at[z], r, down)
    own_p = send(x_ref, own, xs_p.at[z], xp.at[z], r, mate)

    @pl.when(z < chips - 1)
    def _():
        own_up.start()

    @pl.when(z > 0)
    def _():
        own_dn.start()

    own_p.start()
    xall[x_rows(z, c), :] = x_ref[...]

    def block_copies(chip):
        block = xall.at[x_rows(chip, c)]
        return (send(block, block, xs_up.at[chip], xr.at[chip], r, up),
                send(block, block, xs_dn.at[chip], xr.at[chip], r, down),
                send(block, block, xs_p.at[chip], xp.at[chip], r, mate))

    def forward(distance):
        @pl.when(z >= distance)
        def _():
            to_up, _unused, to_mate = block_copies(z - distance)
            to_up.wait_recv()

            @pl.when(z < chips - 1)
            def _():
                to_up.start()

            to_mate.start()

        @pl.when(z + distance < chips)
        def _():
            _unused, to_dn, to_mate = block_copies(z + distance)
            to_dn.wait_recv()

            @pl.when(z > 0)
            def _():
                to_dn.start()

            to_mate.start()

    def part(h):
        return pl.ds(pl.multiple_of(h * dc, dc), dc)

    def pair_copy(h):
        return send(pb.at[1 - c, :, :, part(h)], rb.at[:, :, part(h)], ps.at[h], pr.at[h], r, mate)

    def pair_sum(b, h):
        j = exclusive_or(r, b, rows_n)
        return pb[c, j, :, part(h)].astype(jnp.float32) + rb[j, :, part(h)].astype(jnp.float32)

    def up_copy(b, h):
        return send(sb_up.at[b, :, part(h)], ub.at[b, :, part(h)], us.at[b, h], ur.at[b, h], r, up)

    def dn_copy(b, h):
        return send(sb_dn.at[b, :, part(h)], db.at[b, :, part(h)], ds.at[b, h], dr.at[b, h], r, down)

    def up_step(h):
        def body(i, carry):
            b = chips - 1 - i
            copy = up_copy(b, h)

            @pl.when(z == 0)
            def _():
                sb_up[b, :, part(h)] = pair_sum(b, h).astype(jnp.bfloat16)

            @pl.when(z > 0)
            def _():
                copy.wait_recv()
                sb_up[b, :, part(h)] = (pair_sum(b, h) + ub[b, :, part(h)].astype(jnp.float32)).astype(jnp.bfloat16)

            copy.start()
            return carry

        lax.fori_loop(0, chips - 1 - z, body, 0)

    def dn_step(h):
        def body(b, carry):
            copy = dn_copy(b, h)

            @pl.when(z == chips - 1)
            def _():
                sb_dn[b, :, part(h)] = pair_sum(b, h).astype(jnp.bfloat16)

            @pl.when(z < chips - 1)
            def _():
                copy.wait_recv()
                sb_dn[b, :, part(h)] = (pair_sum(b, h) + db[b, :, part(h)].astype(jnp.float32)).astype(jnp.bfloat16)

            copy.start()
            return carry

        lax.fori_loop(0, z, body, 0)

    def final_step(h):
        total = pair_sum(z, h)

        @pl.when(z > 0)
        def _():
            up_copy(z, h).wait_recv()

        @pl.when(z < chips - 1)
        def _():
            dn_copy(z, h).wait_recv()

        @pl.when(z == 0)
        def _():
            out_ref[:, part(h)] = (total + db[z, :, part(h)].astype(jnp.float32)).astype(jnp.bfloat16)

        @pl.when(z == chips - 1)
        def _():
            out_ref[:, part(h)] = (total + ub[z, :, part(h)].astype(jnp.float32)).astype(jnp.bfloat16)

        @pl.when((z > 0) & (z < chips - 1))
        def _():
            out_ref[:, part(h)] = (total + ub[z, :, part(h)].astype(jnp.float32)
                                   + db[z, :, part(h)].astype(jnp.float32)).astype(jnp.bfloat16)

    tile = min(dc, 512)

    def multiply(h):
        w_copy(h).wait()

        def body(t, carry):
            at = pl.multiple_of(h * dc + t * tile, tile)
            product = lax.dot_general(
                w_v[pl.ds(at, tile), :], gall[...], (((1,), (1,)), ((), ())),
                preferred_element_type=jnp.float32,
            )
            flat = product.T.astype(jnp.bfloat16)
            for j in range(rows_n):
                for core in range(2):
                    first = j * trow + core * tcol
                    pb[core, j, :, pl.ds(at, tile)] = flat[first:first + tcol, :]
            return carry

        lax.fori_loop(0, dc // tile, body, 0)
        pair_copy(h).start()

    for copy, relay in zip(first, second):
        copy.wait_recv()
        relay.start()
    forward(1)
    for copy in first[len(second):] + second:
        copy.wait_recv()

    last = PAIR_LAG + LEVEL_LAG * (chips - 1)
    for slot in range(parts + last):
        if slot < parts:
            multiply(slot)
        if 0 <= slot - PAIR_LAG < parts:
            pair_copy(slot - PAIR_LAG).wait_recv()
        h_up = slot - PAIR_LAG - LEVEL_LAG * z
        h_dn = slot - PAIR_LAG - LEVEL_LAG * (chips - 1 - z)

        @pl.when((h_up >= 0) & (h_up < parts))
        def _():
            up_step(h_up)

        @pl.when((h_dn >= 0) & (h_dn < parts))
        def _():
            dn_step(h_dn)

        if 0 <= slot - last < parts:
            final_step(slot - last)
        if slot == parts // 4:
            for distance in range(2, chips - 1):
                forward(distance)
    if chips > 2:
        forward(chips - 1)

    for copy in first + second:
        copy.wait_send()
    for h in range(parts):
        pair_copy(h).wait_send()
    for chip in range(chips):
        to_up, to_dn, to_mate = block_copies(chip)
        to_mate.wait()

        @pl.when((z >= chip) & (z < chips - 1))
        def _():
            to_up.wait_send()

        @pl.when((z <= chip) & (z > 0))
        def _():
            to_dn.wait_send()

        for h in range(parts):
            @pl.when(z < chip)
            def _():
                up_copy(chip, h).wait_send()

            @pl.when(z > chip)
            def _():
                dn_copy(chip, h).wait_send()


def is_rising(row):
    return row // 2 % 2 == 0


def staged_kernel(rows_n, chips, parts, g_hbm, pos_hbm, x_hbm, w_ref, gall, xall, own_ref, last_ref,
                  w_v, raw, pos_ref, pb, rb, ub, db, sb_up, sb_dn,
                  w_sem, in_sem, gs, gr, xs_up, xs_dn, xs_p, xr, xp, ps, pr, us, ur, ds, dr):
    r = lax.axis_index("row")
    q = lax.axis_index("col")
    z, c = q // 2, q % 2
    mate = z * 2 + 1 - c
    up, down = q + 2, q - 2
    rising = is_rising(r)
    falling = jnp.logical_not(rising)
    trow, width = g_hbm.shape
    tcol, depth = x_hbm.shape
    dc = depth // parts
    pieces = 2
    prow = tcol // pieces

    def x_rows(chip, core, p):
        first = exclusive_or(r, chip, chips) * (2 * tcol) + core * tcol + p * prow
        return pl.ds(pl.multiple_of(first, prow), prow)

    g_in = pltpu.make_async_copy(g_hbm, raw, in_sem.at[0])
    g_in.start()
    pos_in = pltpu.make_async_copy(pos_hbm, pos_ref, in_sem.at[3])
    pos_in.start()
    x_in = [pltpu.make_async_copy(x_hbm.at[pl.ds(p * prow, prow)], xall.at[x_rows(z, c, p)], in_sem.at[1 + p])
            for p in range(pieces)]
    for copy in x_in:
        copy.start()

    barrier = pltpu.get_barrier_semaphore()
    for j in (1, 2):
        pl.semaphore_signal(barrier, inc=1, device_id=(exclusive_or(r, j, rows_n), q), device_id_type=MESH)
    pl.semaphore_signal(barrier, inc=1, device_id=(r, mate), device_id_type=MESH)

    @pl.when(z > 0)
    def _():
        pl.semaphore_signal(barrier, inc=1, device_id=(r, down), device_id_type=MESH)

    @pl.when(z < chips - 1)
    def _():
        pl.semaphore_signal(barrier, inc=1, device_id=(r, up), device_id_type=MESH)

    def w_copy(h):
        rows = pl.ds(pl.multiple_of(h * dc, dc), dc)
        return pltpu.make_async_copy(w_ref.at[rows], w_v.at[rows], w_sem.at[h])

    for h in range(parts):
        w_copy(h).start()

    pos_in.wait()
    g_in.wait()
    unrotate_heads(raw, pos_ref, gall, q * width)
    for copy in x_in:
        copy.wait()

    inner = (z > 0) & (z < chips - 1)

    @pl.when(inner)
    def _():
        pl.semaphore_wait(barrier, 5)

    @pl.when(jnp.logical_not(inner))
    def _():
        pl.semaphore_wait(barrier, 4)

    def send(src, dst, s_sem, r_sem, row, col):
        return pltpu.make_async_remote_copy(
            src_ref=src, dst_ref=dst, send_sem=s_sem, recv_sem=r_sem,
            device_id=(row, col), device_id_type=MESH,
        )

    cut = width // 2
    halves = (slice(0, cut), slice(cut, width))

    def g_copy(j, k):
        return send(gall.at[0:trow, halves[k]], gall.at[j * trow:(j + 1) * trow, halves[k]],
                    gs.at[j, k], gr.at[j, k], exclusive_or(r, j, rows_n), q)

    def g_relay(j):
        k = j - 1
        return send(gall.at[j * trow:(j + 1) * trow, halves[k]], gall.at[3 * trow:4 * trow, halves[k]],
                    gs.at[3, k], gr.at[3, k], exclusive_or(r, 3 - j, rows_n), q)

    g_first = [g_copy(1, 0), g_copy(2, 1)]
    g_second = [g_copy(1, 1), g_copy(2, 0)]
    g_third = [g_relay(1), g_relay(2)]
    for copy in g_first + g_second:
        copy.start()

    def block_copies(chip, p):
        block = xall.at[x_rows(chip, c, p)]
        return (send(block, block, xs_up.at[chip, p], xr.at[chip, p], r, up),
                send(block, block, xs_dn.at[chip, p], xr.at[chip, p], r, down),
                send(block, block, xs_p.at[chip, p], xp.at[chip, p], r, mate))

    for p in range(pieces):
        to_up, to_dn, to_mate = block_copies(z, p)

        @pl.when(z < chips - 1)
        def _():
            to_up.start()

        @pl.when(z > 0)
        def _():
            to_dn.start()

        to_mate.start()

    def forward(distance, p):
        @pl.when(z >= distance)
        def _():
            to_up, _unused, to_mate = block_copies(z - distance, p)
            to_up.wait_recv()

            @pl.when(z < chips - 1)
            def _():
                to_up.start()

            to_mate.start()

        @pl.when(z + distance < chips)
        def _():
            _unused, to_dn, to_mate = block_copies(z + distance, p)
            to_dn.wait_recv()

            @pl.when(z > 0)
            def _():
                to_dn.start()

            to_mate.start()

    def part(h):
        return pl.ds(pl.multiple_of(h * dc, dc), dc)

    def pair_copy(j, h):
        return send(pb.at[1 - c, j, :, part(h)], rb.at[j, :, part(h)], ps.at[j, h], pr.at[j, h], r, mate)

    def pair_sum(j, h):
        return pb[c, j, :, part(h)].astype(jnp.float32) + rb[j, :, part(h)].astype(jnp.float32)

    def up_copy(j, h):
        return send(sb_up.at[j, :, part(h)], ub.at[j, :, part(h)], us.at[j, h], ur.at[j, h], r, up)

    def dn_copy(j, h):
        return send(sb_dn.at[j, :, part(h)], db.at[j, :, part(h)], ds.at[j, h], dr.at[j, h], r, down)

    def multiply(i, first, last):
        h = i % parts
        product = lax.dot_general(
            w_v[part(h), :], gall[first * trow:last * trow, :], (((1,), (1,)), ((), ())),
            preferred_element_type=jnp.float32,
        )
        flat = product.T.astype(half)
        for j in range(first, last):
            for core in range(2):
                at = (j - first) * trow + core * tcol
                pb[core, j, :, part(h)] = flat[at:at + tcol, :]
        for j in range(first, last):
            pair_copy(j, h).start()

    count = 2 * parts + parts // 2
    firsts = [parts * ((j + 3) // 4) + (parts // 2) * (j // 3) for j in range(rows_n)]

    def each_block(slot, lo, hi, lag, act, busy=None, late=None, only=None):
        def block(j, guard=None):
            least, most = firsts[j], firsts[j] + parts
            if hi - lag <= least or lo - lag >= most or only not in (None, j):
                return
            dest = exclusive_or(r, j, rows_n)

            def run():
                act(j, (slot - lag) % parts, dest)

            conds = [] if guard is None else [guard(dest)]
            if lo - lag < least or hi - lag > most:
                conds.append((slot - lag >= least) & (slot - lag < most))
            if conds:
                pl.when(functools.reduce(jnp.logical_and, conds))(run)
            else:
                run()

        last_parts = late is not None and hi - lag > count - parts

        if busy is not False:
            block(3, (lambda dest: dest != late) if last_parts else None)
            block(2, (lambda dest: (dest != late) | (slot - lag < count - parts)) if last_parts else None)
        block(1)
        block(0)
        if last_parts:
            block(3, lambda dest: dest == late)

    def own_step(j, h, dest):
        pair_copy(j, h).wait_recv()

    def chain_step(copy, arrived, sent, busy, ends, origin, near, beyond, here, h, j):
        def total():
            return pair_sum(j, h)

        sends, stays = (beyond, near) if busy else (beyond | near, here)

        def settled(value):
            if ends is not True:
                @pl.when(sends)
                def _():
                    sent[j, :, part(h)] = value.astype(half)
                    copy.start()

            if ends is not False:
                @pl.when(stays)
                def _():
                    if busy:
                        last_ref[:, part(h)] = value.astype(half)
                    else:
                        own_ref[:, part(h)] = value

        takes = sends | stays if ends is None else stays if ends else sends

        @pl.when(takes & jnp.logical_not(origin))
        def _():
            copy.wait_recv()
            settled(total() + arrived[j, :, part(h)].astype(jnp.float32))

        @pl.when((takes & origin))
        def _():
            settled(total())

    def up_step(busy, ends, j, h, dest):
        chain_step(up_copy(j, h), ub, sb_up, busy, ends, z == 0, dest == z + 1, dest > z + 1, dest == z, h, j)

    def dn_step(busy, ends, j, h, dest):
        chain_step(dn_copy(j, h), db, sb_dn, busy, ends, z == chips - 1, dest == z - 1, dest < z - 1, dest == z, h, j)

    late_up, late_dn = 2, chips - 3

    def settle_late(chip):
        for busy, late, at, act in ((rising, late_up, chip, up_step), (falling, late_dn, chips - 1 - chip, dn_step)):
            for i in range(count - parts, 2 * parts):
                dest = exclusive_or(r, 2, rows_n)

                @pl.when((z == at) & (dest == late) & busy)
                def _():
                    act(True, None, 2, i % parts, dest)

    def settle_short(chip, products):
        for idle, at, act in ((falling, chip, up_step), (rising, chips - 1 - chip, dn_step)):
            @pl.when((z == at) & idle)
            def _():
                for i in products:
                    for j in (2, 3):
                        if firsts[j] <= i < firsts[j] + parts:
                            act(False, None, j, i % parts, exclusive_or(r, j, rows_n))

    def settle(slot, lo, hi, ends=None, pairs=True, chain=None):
        if pairs and not ends:
            each_block(slot, lo, hi, 1, own_step)
        for chip in range(chips) if chain is None else chain:
            lag_up, lag_dn = 1 + CHAIN_LAG * chip, 1 + CHAIN_LAG * (chips - 1 - chip)
            near_up, near_dn = 1 + NEAR_LAG * chip, 1 + NEAR_LAG * (chips - 1 - chip)
            ups = hi > lag_up and lo < count + lag_up
            dns = hi > lag_dn and lo < count + lag_dn
            @pl.when((z == chip) & rising)
            def _():
                for j, lag in ((1, near_dn), (0, lag_dn)):
                    each_block(slot, lo, hi, lag, functools.partial(dn_step, False, ends), False, only=j)
                if ups:
                    each_block(slot, lo, hi, lag_up, functools.partial(up_step, True, ends), True, late_up)

            @pl.when((z == chip) & falling)
            def _():
                for j, lag in ((1, near_up), (0, lag_up)):
                    each_block(slot, lo, hi, lag, functools.partial(up_step, False, ends), False, only=j)
                if dns:
                    each_block(slot, lo, hi, lag_dn, functools.partial(dn_step, True, ends), True, late_dn)

    def products(start, stop, first, last, after):
        def body(i, carry):
            if start == 0:
                w_copy(i).wait()
            multiply(i, first, last)
            for at, act in after:
                pl.when(i == at)(act)
            settle(i, start, stop)
            return carry

        lax.fori_loop(start, stop, body, 0)

    def early():
        for copy, relay in zip(g_first, g_third):
            copy.wait_recv()
            relay.start()
        forward(1, 0)

    half_way = parts // 2
    products(0, parts, 0, 1, [(parts - 2, early), (parts - 1, lambda: forward(1, 1))])
    for copy in g_second:
        copy.wait_recv()
    products(parts, parts + half_way, 1, 3, [(parts + half_way - 1, lambda: forward(2, 0))])
    for copy in g_third:
        copy.wait_recv()
    products(parts + half_way, 2 * parts, 1, 4, [(parts + half_way, lambda: forward(2, 1))])
    products(2 * parts, 2 * parts + half_way, 3, 4, [(2 * parts, lambda: forward(3, 0))])

    @pl.when((rising & (z == chips - 1)) | (falling & (z == 0)))
    def _():
        last_ref[...] = jnp.zeros_like(last_ref)

    settle_short(0, range(parts, count - 1))
    for slot in range(count, count + 1 + CHAIN_LAG * (chips - 1)):
        if slot == count:
            settle(slot, slot, slot + 1, False, False, range(1, chips - 1))
            settle(slot, slot, slot + 1, False, True, (0, chips - 1))
            forward(3, 1)
        else:
            settle(slot, slot, slot + 1, False)
        if slot == count:
            settle_short(0, [count - 1])
            settle_late(0)
    for copy in g_first + g_second + g_third:
        copy.wait_send()
    for chip in range(chips):
        for p in range(pieces):
            to_up, to_dn, to_mate = block_copies(chip, p)
            to_mate.wait()

            @pl.when((z >= chip) & (z < chips - 1))
            def _():
                to_up.wait_send()

            @pl.when((z <= chip) & (z > 0))
            def _():
                to_dn.wait_send()

    def swapped(j, carry):
        for h in range(parts):
            pair_copy(j, h).wait_send()
        return carry

    lax.fori_loop(0, rows_n, swapped, 0)

    for slot in range(count, count + 1 + CHAIN_LAG * (chips - 1)):
        settle(slot, slot, slot + 1, True)
    settle_late(1)
    settle_short(1, range(parts, count))

    def sent(j, carry):
        dest = exclusive_or(r, j, rows_n)
        for h in range(parts):
            @pl.when((dest > z + 1) | (falling & (dest == z + 1)))
            def _():
                up_copy(j, h).wait_send()

            @pl.when((dest < z - 1) | (rising & (dest == z - 1)))
            def _():
                dn_copy(j, h).wait_send()
        return carry

    lax.fori_loop(0, rows_n, sent, 0)


def outer_kernel(x_ref, g_ref, out_ref, buf, sem):
    slots, block, _ = buf.shape
    steps = out_ref.shape[0] // block

    def rows(i):
        return pl.ds(pl.multiple_of(i * block, block), block)

    def out_copy(i):
        slot = lax.rem(i, slots)
        return pltpu.make_async_copy(buf.at[slot], out_ref.at[rows(i)], sem.at[slot])

    def body(i, carry):
        @pl.when(i >= slots)
        def _():
            out_copy(i - slots).wait()

        buf[lax.rem(i, slots), :, :] = lax.dot_general(
            x_ref[:, rows(i)], g_ref[...], (((0,), (0,)), ((), ())), preferred_element_type=jnp.float32
        )
        out_copy(i).start()
        return carry

    lax.fori_loop(0, steps, body, 0)
    for i in range(steps - slots, steps):
        out_copy(i).wait()


def outer_streamed(left, right):
    tokens, depth = left.shape
    width = right.shape[1]
    block, slots = 2 * HEAD, 4
    vmem = pl.BlockSpec(memory_space=pltpu.VMEM)
    return pl.pallas_call(
        outer_kernel,
        out_shape=jax.ShapeDtypeStruct((depth, width), jnp.float32),
        in_specs=[vmem, vmem],
        out_specs=pl.BlockSpec(memory_space=pltpu.HBM),
        scratch_shapes=[pltpu.VMEM((slots, block, width), jnp.float32), pltpu.SemaphoreType.DMA((slots,))],
        compiler_params=pltpu.CompilerParams(vmem_limit_bytes=24 * 2**20),
        cost_estimate=pl.CostEstimate(
            flops=2 * tokens * depth * width, bytes_accessed=4 * depth * width, transcendentals=0
        ),
    )(left, right)


def staged(rows_n, chips, inputs, weight, grad_out, positions):
    depth, width = weight.shape
    trow, tcol = grad_out.shape[0], inputs.shape[0]
    parts = 4
    dma = pltpu.SemaphoreType.DMA
    vmem = pl.BlockSpec(memory_space=pltpu.VMEM)
    hbm = pl.BlockSpec(memory_space=pltpu.HBM)
    whole_grad, whole_inputs, own, last = pl.pallas_call(
        functools.partial(staged_kernel, rows_n, chips, parts),
        out_shape=(
            jax.ShapeDtypeStruct((rows_n * trow, width), half),
            jax.ShapeDtypeStruct((chips * 2 * tcol, depth), half),
            jax.ShapeDtypeStruct((tcol, depth), jnp.float32),
            jax.ShapeDtypeStruct((tcol, depth), half),
        ),
        in_specs=[hbm] * 4,
        out_specs=(vmem,) * 4,
        scratch_shapes=[
            pltpu.VMEM((depth, width), half),
            pltpu.VMEM((trow, width), half),
            pltpu.VMEM((1, trow), jnp.int32),
            pltpu.VMEM((2, rows_n, tcol, depth), half),
            pltpu.VMEM((rows_n, tcol, depth), half),
            pltpu.VMEM((rows_n, tcol, depth), half),
            pltpu.VMEM((rows_n, tcol, depth), half),
            pltpu.VMEM((rows_n, tcol, depth), half),
            pltpu.VMEM((rows_n, tcol, depth), half),
            dma((parts,)), dma((4,)),
            dma((rows_n, 2)), dma((rows_n, 2)),
            dma((chips, 2)), dma((chips, 2)), dma((chips, 2)), dma((chips, 2)), dma((chips, 2)),
            dma((rows_n, parts)), dma((rows_n, parts)),
            dma((rows_n, parts)), dma((rows_n, parts)), dma((rows_n, parts)), dma((rows_n, parts)),
        ],
        compiler_params=pltpu.CompilerParams(
            collective_id=0, has_side_effects=True, vmem_limit_bytes=44 * 2**20
        ),
        cost_estimate=pl.CostEstimate(
            flops=2 * rows_n * trow * width * depth, bytes_accessed=2 * width * depth, transcendentals=0
        ),
    )(*(pltpu.with_memory_space_constraint(a, pltpu.HBM) for a in (grad_out, positions[None, :], inputs, weight)))
    cols = 2 * chips
    hops = [(row * cols + q, row * cols + q + 2) for row in range(rows_n) for q in range(cols - 2)]
    hops = [(a, b) if is_rising(a // cols) else (b, a) for a, b in hops]
    arrived = lax.ppermute(last, ("row", "col"), hops)
    weight_grad = outer_streamed(whole_inputs, whole_grad)
    input_grad = (own + arrived.astype(jnp.float32)).astype(half)
    return (input_grad, weight_grad)


def outer_sum(left, right):
    return lax.dot_general(
        left, right, (((0,), (0,)), ((), ())), preferred_element_type=jnp.float32
    )


def per_device(rows_n, chips, inputs, weight, grad_out, positions):
    depth, width = weight.shape
    trow, tcol = grad_out.shape[0], inputs.shape[0]
    if rows_n == 4 and chips == 4 and width % (2 * HEAD) == 0 and depth % (8 * HEAD) == 0 and trow == 2 * tcol:
        return staged(rows_n, chips, inputs, weight, grad_out, positions)
    col_start = lax.axis_index("col") * width
    raw = width % HEAD == 0
    grad = grad_out if raw else unrotate(grad_out, positions, col_start)
    parts = 8 if depth % (8 * HEAD) == 0 else 4
    dma = pltpu.SemaphoreType.DMA
    vmem = pl.BlockSpec(memory_space=pltpu.VMEM)
    whole_grad, whole_inputs, input_grad = pl.pallas_call(
        functools.partial(kernel, rows_n, chips, parts, raw),
        out_shape=(
            jax.ShapeDtypeStruct((rows_n * trow, width), half),
            jax.ShapeDtypeStruct((chips * 2 * tcol, depth), half),
            jax.ShapeDtypeStruct((tcol, depth), half),
        ),
        in_specs=[vmem, vmem, vmem, pl.BlockSpec(memory_space=pl.ANY)],
        out_specs=(vmem, vmem, vmem),
        scratch_shapes=[
            pltpu.VMEM((depth, width), half),
            pltpu.VMEM((2, rows_n, tcol, depth), half),
            pltpu.VMEM((rows_n, tcol, depth), half),
            pltpu.VMEM((chips, tcol, depth), half),
            pltpu.VMEM((chips, tcol, depth), half),
            pltpu.VMEM((chips, tcol, depth), half),
            pltpu.VMEM((chips, tcol, depth), half),
            dma((parts,)),
            dma((rows_n, 2)), dma((rows_n, 2)),
            dma((chips,)), dma((chips,)), dma((chips,)), dma((chips,)), dma((chips,)),
            dma((parts,)), dma((parts,)),
            dma((chips, parts)), dma((chips, parts)), dma((chips, parts)), dma((chips, parts)),
        ],
        compiler_params=pltpu.CompilerParams(
            collective_id=0, has_side_effects=True, vmem_limit_bytes=60 * 2**20
        ),
        cost_estimate=pl.CostEstimate(
            flops=2 * rows_n * trow * width * depth, bytes_accessed=2 * width * depth, transcendentals=0
        ),
    )(grad, positions[None, :], inputs, weight)
    weight_grad = outer_sum(whole_inputs, whole_grad)
    return (input_grad, weight_grad)


def solution(mesh):
    rows_n, chips = mesh.shape["row"], mesh.shape["col"] // 2
    in_specs = (P("col", "row"), P("row", "col"), P("row", "col"), P("row"))
    out_specs = (P("col", "row"), P("row", "col"))
    return jax.shard_map(
        functools.partial(per_device, rows_n, chips), mesh=mesh, in_specs=in_specs,
        out_specs=out_specs, check_vma=False,
    )
```
